128 devices in a mesh: ex: 4 (over y), ft: 32 (over x, z, core).
Axes of the slice: x: 4, y: 4, z: 4, core: 2. Of those that a mesh axis runs over, the one named last changes fastest.
Arguments:
- features: bfloat16 [2048, 262144], P(('ex', 'ft')), may hold values from -0.046875 to 0.046875
- labels: int32 [2048], P(('ex', 'ft')), may hold values 0 or 1
- start_weights: float32 [262144], P(('ex', 'ft')), may hold values from -6 to 6
- hist_s: float32 [20, 262144], P(None, ('ex', 'ft')), may hold values from -12 to 12
- hist_y: float32 [20, 262144], P(None, ('ex', 'ft')), may hold values from -30 to 30, as said below
Outputs:
- new_weights: float32 [262144], P(('ex', 'ft'))
- direction: float32 [262144], P(('ex', 'ft'))
The draws below stay inside these ranges and needn't reach their ends.
Inputs may be any that keep to these rules, and one draw needn't show every extreme that they name: Entry by entry, hist_y times hist_s is nonnegative, and every pair has a positive inner product; every entry of hist_y is at most 1.2 times the matching entry of hist_s in magnitude.
All inputs are finite; a program needn't handle non-finite values. No bound on the sum of `labels` on one device may be relied on, other than what follows from the above.
Results may differ from the reference program's by a relative error of at most 0.0081.
Values may be sent and summed in bfloat16 or wider, within the bound.
A program may use at most 64 MiB of HBM per device.

```python
import jax
import jax.numpy as jnp
from jax import lax

F = 262144
HIST = 20
ITERS = 2
EXAMPLES = 2048


def history_pair(key):
    base = jax.random.fold_in(key, 11)
    key_s, key_c, key_u, key_b = jax.random.split(base, 4)
    block_scale = jnp.exp(jax.random.uniform(key_b, (HIST, F // 128), jnp.float32, jnp.log(0.3), jnp.log(3.0)))
    block_scale = jnp.repeat(block_scale, 128, axis=1)
    plain = jnp.clip(jax.random.normal(key_s, (HIST, F), jnp.float32), -4.0, 4.0)
    curve = jnp.exp(jax.random.uniform(key_c, (HIST, F), jnp.float32, jnp.log(0.35), jnp.log(1.0)))
    steps = plain * block_scale
    noise = jax.random.uniform(key_u, (HIST, F), jnp.float32, -1.0, 1.0)
    diffs = curve * steps + 0.2 * curve * noise * jnp.abs(steps)
    return (steps, diffs)


def draw_hist_s(key, part):
    return history_pair(key)[0]


def draw_hist_y(key, part):
    return history_pair(key)[1]


def place_ends(result, rng, least, largest):
    longest = result.shape.index(max(result.shape))
    spots = []
    for shift in (0, 1):
        where = [jax.random.randint(jax.random.fold_in(rng, axis), (), 0, length) for axis, length in enumerate(result.shape)]
        where[longest] = (where[longest] + shift) % result.shape[longest]
        spots.append(tuple(where))
    return result.at[spots[0]].set(least).at[spots[1]].set(largest)


def raised(result, own_key, source, target, parts, factor):
    owner, partner = [(jnp.arange(result.shape[axis_at]) // (result.shape[axis_at] // parts)).reshape([-1 if axis == axis_at else 1 for axis in range(result.ndim)]) for axis_at in (source, target)]
    chosen = jax.random.permutation(own_key, parts)[partner]
    strong = (owner == chosen) | (owner == (partner + parts // 2) % parts)
    return jnp.where(strong, factor * result, result)


def levels(key, extent, shards, low, high):
    def one(dim, blocks):
        draws = jax.random.uniform(jax.random.fold_in(jax.random.fold_in(key, 6), dim), (blocks,), jnp.float32, low / len(shards), high / len(shards))
        return jnp.repeat(jnp.exp(draws), extent[dim] // blocks).reshape((-1,) + (1,) * (len(extent) - dim - 1))

    level = one(*shards[0])
    for cut in shards[1:]:
        level = level * one(*cut)
    return level


def normal_values(rng, dims, scale, reach, shards=(), kind=jnp.bfloat16):
    result = scale * jax.random.normal(rng, dims, jnp.float32)
    if shards:
        result = result * levels(rng, dims, shards, -0.22, 0.18)
    return jnp.clip(result, -reach, reach).astype(kind)


def gaussian_with(stream_key, dims, deviation, reach, cuts, heavy, dtype=jnp.bfloat16):
    result = deviation * jax.random.normal(stream_key, dims, jnp.float32)
    if cuts:
        result = result * levels(stream_key, dims, cuts, -0.22, 0.18)
    return jnp.clip(raised(result, jax.random.fold_in(stream_key, 3), *heavy), -reach, reach).astype(dtype)


def setup_inputs(seed: int = 0) -> dict:
    arg_keys = jax.random.split(jax.random.key(seed), 6)
    return {
        "features": gaussian_with(arg_keys[0], (EXAMPLES, F), F ** -0.5, 0.046875, ((0, 128),), (0, 1, 128, 5.5)),
        "labels": place_ends((jax.random.randint(arg_keys[1], (EXAMPLES,), 0, 2) < 1).astype(jnp.int32), jax.random.fold_in(arg_keys[1], 1), 0, 1),
        "start_weights": normal_values(arg_keys[2], (F,), 1.0, 6.0, ((0, 128),), jnp.float32),
        "hist_s": draw_hist_s(jax.random.fold_in(arg_keys[5], 71), 0),
        "hist_y": draw_hist_y(jax.random.fold_in(arg_keys[5], 71), 0),
    }


def two_loop(gram):
    pairs = (gram.shape[0] - 1) // 2
    delta = jnp.zeros((gram.shape[0],), jnp.float32).at[2 * pairs].set(-1.0)
    alphas = [None] * pairs
    for index in reversed(range(pairs)):
        alpha = jnp.sum(delta * gram[:, index]) / gram[index, pairs + index]
        delta = delta.at[pairs + index].add(-alpha)
        alphas[index] = alpha
    delta = delta * (gram[pairs - 1, 2 * pairs - 1] / gram[2 * pairs - 1, 2 * pairs - 1])
    for index in range(pairs):
        beta = jnp.sum(delta * gram[pairs + index, :]) / gram[index, pairs + index]
        delta = delta.at[index].add(alphas[index] - beta)
    return delta


def reference(features, labels, start_weights, hist_s, hist_y):
    weights = start_weights
    stored_s, stored_y = hist_s, hist_y
    prev_weights = weights
    prev_grad = weights
    direction = weights
    for step in range(ITERS):
        margin = jnp.dot(features, weights.astype(jnp.bfloat16), preferred_element_type=jnp.float32)
        resid = (jax.nn.sigmoid(margin) - labels.astype(jnp.float32)).astype(jnp.bfloat16)
        grad = jnp.dot(resid, features, preferred_element_type=jnp.float32) + 0.1 * weights
        if step > 0:
            stored_s = jnp.concatenate([stored_s[1:], (weights - prev_weights)[None]], axis=0)
            stored_y = jnp.concatenate([stored_y[1:], (grad - prev_grad)[None]], axis=0)
        basis = jnp.concatenate([stored_s, stored_y, grad[None]], axis=0)
        gram = jnp.dot(basis, basis.T, precision=lax.Precision.HIGHEST, preferred_element_type=jnp.float32)
        delta = two_loop(gram)
        direction = jnp.dot(delta, basis, precision=lax.Precision.HIGHEST, preferred_element_type=jnp.float32)
        prev_weights, prev_grad = weights, grad
        weights = weights + direction
    return weights, direction
```

```python
import functools

import jax
import jax.numpy as jnp
from jax import lax
from jax.experimental import pallas as pl
from jax.experimental.pallas import tpu as pltpu
from jax.sharding import PartitionSpec as P

ITERS = 2
MESH = pl.DeviceIdType.MESH
HI = lax.Precision.HIGHEST
F32 = jnp.float32
BF16 = jnp.bfloat16


def contract_last(a, b):
    return lax.dot_general(a, b, (((1,), (1,)), ((), ())), precision=HI, preferred_element_type=F32)


def kernel(
    sizes, x_hbm, lab_ref, w_ref, s_hbm, y_hbm, wout_ref, dout_ref,
    x_v, s_v, y_v, wg, rs_send, rs_recv, ar, gl, gtmp, gcore, gax,
    lab_send, lab_recv, m_send, m_recv, r_ref, acc_ref, t_ref, g_ref, gp_ref, d_ref,
    x_sem, xr_send, xr_recv, h_sem, ag_send, ag_recv, rs_ssem, rs_rsem,
    ar_ssem, ar_rsem, g_ssem, g_rsem, l_sem, m_ssem, m_rsem,
):
    ny, nx, nz = sizes
    plane = nx * nz
    chips = ny * plane
    m = s_v.shape[0]
    ex = lax.axis_index("ex")
    ft = lax.axis_index("ft")
    core = lax.rem(ft, 2)
    xz = ft // 2
    px, pz = xz // nz, lax.rem(xz, nz)
    chip = ex * plane + xz
    me = chip * 2 + core
    other = 1 - core

    def peer(oy, ox, oz):
        cy = lax.rem(ex + oy, ny)
        cx = lax.rem(px + ox, nx)
        cz = lax.rem(pz + oz, nz)
        return cy, cx * nz + cz

    hist = [
        pltpu.make_async_copy(s_hbm, s_v, h_sem.at[0]),
        pltpu.make_async_copy(y_hbm, y_v, h_sem.at[1]),
    ]
    for copy in hist:
        copy.start()
    local = []
    for h in range(2):
        copy = pltpu.make_async_copy(x_hbm.at[h, :, core], x_v.at[:, core * 2 + h], x_sem.at[h])
        copy.start()
        local.append(copy)

    barrier = pltpu.get_barrier_semaphore()

    def greet(k, carry):
        oy, ox, oz = k // plane, lax.rem(k // nz, nx), lax.rem(k, nz)
        cy, cxz = peer(oy, ox, oz)
        pl.semaphore_signal(barrier, inc=1, device_id=(cy, cxz * 2 + core), device_id_type=MESH)
        return carry

    pl.semaphore_signal(barrier, inc=1, device_id=(ex, xz * 2 + other), device_id_type=MESH)
    lax.fori_loop(1, chips, greet, 0)

    row8 = lax.broadcasted_iota(jnp.int32, (8, 128), 0)
    lane8 = lax.rem(lax.broadcasted_iota(jnp.int32, (8, 128), 1), 8)
    lab = jnp.zeros((8, 128), F32)
    for h in range(2):
        for e in range(8):
            value = lab_ref[h * 8 + e].astype(F32)
            lab = jnp.where((row8 == core * 2 + h) & (lane8 == e), value, lab)
    lab_send[...] = lab
    wg[0, chip] = w_ref[...].astype(BF16)
    acc_ref[...] = jnp.zeros_like(acc_ref)
    t_ref[...] = jnp.zeros_like(t_ref)
    gl[...] = jnp.zeros_like(gl)
    m_send[...] = jnp.zeros_like(m_send)
    gtmp[...] = jnp.zeros_like(gtmp)
    pl.semaphore_wait(barrier, chips)

    def gather_copy(it, cy, cxz):
        return pltpu.make_async_remote_copy(
            src_ref=wg.at[it, chip], dst_ref=wg.at[it, chip],
            send_sem=ag_send.at[it], recv_sem=ag_recv.at[it],
            device_id=(cy, cxz * 2 + core), device_id_type=MESH)

    def loop_far(fn):
        def body(k, carry):
            oy = far_off(k // plane, ny)
            ox = far_off(lax.rem(k // nz, nx), nx)
            oz = far_off(lax.rem(k, nz), nz)
            fn(oy, ox, oz)
            return carry
        lax.fori_loop(0, chips - 1, body, 0)

    def far_off(digit, n):
        if n == 4:
            half = digit // 2
            return (digit + 2) * (1 - half) + (3 - digit) * half
        return n - 1 - digit

    def gather_start(it):
        def fn(oy, ox, oz):
            cy, cxz = peer(oy, ox, oz)
            gather_copy(it, cy, cxz).start()
        loop_far(fn)

    def whole(ref, sem):
        return pltpu.make_async_copy(ref, ref, sem)

    gather_start(0)

    remote = []
    for h in range(2):
        copy = pltpu.make_async_remote_copy(
            src_ref=x_hbm.at[h, :, other], dst_ref=x_v.at[:, core * 2 + h],
            send_sem=xr_send.at[h], recv_sem=xr_recv.at[h],
            device_id=(ex, xz * 2 + other), device_id_type=MESH)
        copy.start()
        remote.append(copy)
    lab_copy = pltpu.make_async_remote_copy(
        src_ref=lab_send, dst_ref=lab_recv, send_sem=l_sem.at[0], recv_sem=l_sem.at[1],
        device_id=(ex, xz * 2 + other), device_id_type=MESH)
    lab_copy.start()

    for copy in hist:
        copy.wait()
    gl[0:m, 0:m] = contract_last(s_v[...], y_v[...])
    gtmp[0:m, 0:m] = contract_last(y_v[...], y_v[...])

    def gram_send(stage):
        copies = []
        if stage == 0:
            copies.append(pltpu.make_async_remote_copy(
                src_ref=gcore.at[core], dst_ref=gcore.at[core],
                send_sem=g_ssem.at[0, 0], recv_sem=g_rsem.at[0, 0],
                device_id=(ex, xz * 2 + other), device_id_type=MESH))
        else:
            n = (ny, nx, nz)[stage - 1]
            mine = (ex, px, pz)[stage - 1]
            for off in range(1, n):
                offs = [0, 0, 0]
                offs[stage - 1] = off
                cy, cxz = peer(*offs)
                copies.append(pltpu.make_async_remote_copy(
                    src_ref=gax.at[stage - 1, mine], dst_ref=gax.at[stage - 1, mine],
                    send_sem=g_ssem.at[stage, off - 1], recv_sem=g_rsem.at[stage, off - 1],
                    device_id=(cy, cxz * 2 + core), device_id_type=MESH))
        for copy in copies:
            copy.start()
        return copies

    def gram_sum(stage):
        if stage == 0:
            return gcore[0] + gcore[1]
        n = (ny, nx, nz)[stage - 1]
        total = gax[stage - 1, 0]
        for index in range(1, n):
            total = total + gax[stage - 1, index]
        return total

    gcore[core] = gl[...] + pltpu.roll(gtmp[...], 64, 1)
    gram = gram_send(0)
    gathered = chips - 1
    for copy in gram:
        copy.wait()
    gax[0, ex] = gram_sum(0)
    gram = gram_send(1)
    lab_copy.wait()

    def margins(it):
        group = min(8, chips)

        def body(k, acc):
            for j in range(group):
                c = k * group + j
                xs = x_v[c].reshape(512, 128)
                acc = acc + lax.dot_general(
                    wg[it, c], xs, (((1,), (1,)), ((), ())), preferred_element_type=F32)
            return acc
        return lax.fori_loop(0, chips // group, body, jnp.zeros((16, 512), F32))

    row16 = lax.broadcasted_iota(jnp.int32, (16, 128), 0)
    tile16 = lax.broadcasted_iota(jnp.int32, (16, 128), 1) // 8
    on_diag = row16 == tile16
    row24 = lax.broadcasted_iota(jnp.int32, (24, 128), 0)
    lane24 = lax.broadcasted_iota(jnp.int32, (24, 128), 1)
    lane1 = lax.broadcasted_iota(jnp.int32, (1, 128), 1)
    eye = jnp.where((row24 == lane24) & (row24 < m), 1.0, 0.0).astype(F32)

    weights = w_ref[...]
    rinv = rinvt = yy = diag = gamma0 = None
    for it in range(ITERS):
        whole(wg.at[it, pl.ds(0, gathered)], ag_recv.at[it]).wait()
        if it == 0:
            for copy in local:
                copy.wait()
            for copy in remote:
                copy.wait_recv()
        acc = margins(it)
        for k in range(4):
            part = jnp.where(on_diag, acc[:, k * 128:(k + 1) * 128], 0.0)
            m_send[it, k:k + 1, :] = jnp.sum(part, axis=0, keepdims=True)
        part = m_send[it]
        for shift in (8, 16, 32, 64):
            part = part + pltpu.roll(part, shift, 1)
        m_send[it] = part
        m_copy = pltpu.make_async_remote_copy(
            src_ref=m_send.at[it], dst_ref=m_recv.at[it],
            send_sem=m_ssem.at[it], recv_sem=m_rsem.at[it],
            device_id=(ex, xz * 2 + other), device_id_type=MESH)
        m_copy.start()
        if it == 0:
            for copy in gram:
                copy.wait()
            gax[1, px] = gram_sum(1)
            gram = gram_send(2)
        m_copy.wait()
        margin = m_send[it] + m_recv[it]
        resid = jax.nn.sigmoid(margin) - (lab_send[...] + lab_recv[...])
        for k in range(4):
            spread = jnp.where(on_diag, jnp.broadcast_to(resid[k:k + 1, :], (16, 128)), 0.0)
            r_ref[:, k * 128:(k + 1) * 128] = spread.astype(BF16)

        def scatter_copy(cy, cxz):
            c = cy * plane + cxz
            return pltpu.make_async_remote_copy(
                src_ref=rs_send.at[it, c], dst_ref=rs_recv.at[it, chip],
                send_sem=rs_ssem.at[it], recv_sem=rs_rsem.at[it],
                device_id=(cy, cxz * 2 + core), device_id_type=MESH)

        def scatter(k, carry):
            oy = far_off(k, ny)
            places = []
            for j in range(plane):
                ox, oz = far_off(j // nz, nx), far_off(j % nz, nz)
                cy, cxz = peer(oy, ox, oz)
                places.append((cy, cxz))
                c = cy * plane + cxz
                term = jnp.dot(r_ref[...], x_v[c].reshape(512, 128), preferred_element_type=F32)
                rs_send[it, c] = term.astype(BF16)
            for j, (cy, cxz) in enumerate(places):
                if j < plane - 1:
                    scatter_copy(cy, cxz).start()
                else:
                    @pl.when(k < ny - 1)
                    def _():
                        scatter_copy(cy, cxz).start()
            return carry

        lax.fori_loop(0, ny, scatter, 0)
        rs_recv[it, chip] = rs_send[it, chip]
        if it == 0:
            for copy in gram:
                copy.wait()
            gax[2, pz] = gram_sum(2)
            gram = gram_send(3)
            for copy in gram:
                copy.wait()
            total = gram_sum(3)
            upper = jnp.where((row24 <= lane24) & (lane24 < m), total, 0.0)
            yy = jnp.where((lane24 < m) & (row24 < m), pltpu.roll(total, 64, 1), 0.0)
            diag = upper * eye
            inv = eye
            for i in reversed(range(m)):
                line = inv[i:i + 1, :] / upper[i:i + 1, i:i + 1]
                column = jnp.where(row24[:, 0:1] < i, upper[:, i:i + 1], 0.0)
                inv = jnp.where(row24 == i, line, inv - column * line)
            rinv = inv
            t_ref[0:24, :] = inv
            rinvt = t_ref[...].T[0:24, :]
            gamma0 = upper[m - 1:m, m - 1:m] / yy[m - 1:m, m - 1:m]
        whole(rs_recv.at[it, pl.ds(0, gathered)], rs_rsem.at[it]).wait()

        def add(k, total):
            return total + rs_recv[it, k].astype(F32)
        grad = lax.fori_loop(0, chips, add, jnp.zeros((16, 128), F32), unroll=8) + 0.1 * weights
        g_ref[...] = grad
        vectors = [g_ref]
        if it > 0:
            gp_ref[...] = grad - gp_ref[...]
            vectors.append(gp_ref)
            for t in range(16):
                y_v[0:1, t * 128:(t + 1) * 128] = gp_ref[t:t + 1, :]
        for v, vec in enumerate(vectors):
            acc_s = jnp.zeros((m, 128), F32)
            acc_y = jnp.zeros((m, 128), F32)
            for t in range(16):
                line = vec[t:t + 1, :]
                acc_s = acc_s + s_v[:, t * 128:(t + 1) * 128] * line
                acc_y = acc_y + y_v[:, t * 128:(t + 1) * 128] * line
            acc_ref[v * 64:v * 64 + m, :] = acc_s
            acc_ref[v * 64 + 32:v * 64 + 32 + m, :] = acc_y
        sums = contract_last(jnp.ones((8, 128), F32), acc_ref[...])
        ar[it, me] = sums[0:1, :]

        def total_copy(cy, cxz, co):
            return pltpu.make_async_remote_copy(
                src_ref=ar.at[it, me], dst_ref=ar.at[it, me],
                send_sem=ar_ssem.at[it], recv_sem=ar_rsem.at[it],
                device_id=(cy, cxz * 2 + co), device_id_type=MESH)

        def to_both(oy, ox, oz):
            cy, cxz = peer(oy, ox, oz)
            total_copy(cy, cxz, core).start()
            total_copy(cy, cxz, other).start()
        loop_far(to_both)
        total_copy(ex, xz, other).start()
        whole(ar.at[it, pl.ds(0, 2 * chips - 1)], ar_rsem.at[it]).wait()
        tot = jnp.broadcast_to(jnp.sum(ar[it], axis=0), (8, 128))
        u, hh = tot[0:1], pltpu.roll(tot, 96, 1)[0:1]
        if it == 0:
            gamma = gamma0
            alpha = -jnp.sum(rinv * u, axis=1, keepdims=True)
            p = gamma * (jnp.sum(yy * alpha, axis=0, keepdims=True) + hh)
            p = p + jnp.sum(diag * alpha, axis=0, keepdims=True)
            coef = jnp.sum(rinvt * p, axis=1, keepdims=True)
        else:
            v, z = pltpu.roll(tot, 64, 1)[0:1], pltpu.roll(tot, 32, 1)[0:1]
            v0, z0 = v[:, 0:1], z[:, 0:1]
            gamma = v0 / z0
            old = (row24 > 0) & (lane24 > 0)
            a0 = -u[:, 0:1] / v0
            alpha = -jnp.sum(jnp.where(old, rinv, 0.0) * (u + v * a0), axis=1, keepdims=True)
            alpha = jnp.where(row24[:, 0:1] == 0, a0, alpha)
            along = jnp.sum(eye * alpha, axis=0, keepdims=True)
            newest = jnp.sum(jnp.where(lane1 < m, z, 0.0) * along, axis=1, keepdims=True)
            q = jnp.sum(jnp.where(old, yy, 0.0) * alpha, axis=0, keepdims=True) + z * a0
            q = jnp.where(lane1 == 0, newest, q)
            da = jnp.where(lane1 == 0, v0 * a0, jnp.sum(diag * alpha, axis=0, keepdims=True))
            p = gamma * (q + hh) + da
            coef = jnp.sum(jnp.where(old, rinvt, 0.0) * p, axis=1, keepdims=True)
            along = jnp.sum(eye * coef, axis=0, keepdims=True)
            rest = jnp.sum(jnp.where((lane1 > 0) & (lane1 < m), v, 0.0) * along, axis=1, keepdims=True)
            c0 = (p[:, 0:1] - rest) / v0
            coef = jnp.where(row24[:, 0:1] == 0, c0, coef)
        cs, cy_ = coef[0:m], (-gamma * alpha)[0:m]
        for t in range(16):
            cols = slice(t * 128, (t + 1) * 128)
            d_ref[t:t + 1, :] = jnp.sum(cs * s_v[:, cols] + cy_ * y_v[:, cols], axis=0, keepdims=True)
        direction = d_ref[...] - gamma * g_ref[...]
        new = weights + direction
        if it < ITERS - 1:
            wg[it + 1, chip] = new.astype(BF16)
            gather_start(it + 1)
            gp_ref[...] = grad
            d_ref[...] = new - weights
            for t in range(16):
                s_v[0:1, t * 128:(t + 1) * 128] = d_ref[t:t + 1, :]
            weights = new
        else:
            wout_ref[...] = new
            dout_ref[...] = direction

    for copy in remote:
        copy.wait_send()
    for it in range(ITERS):
        whole(wg.at[it, pl.ds(0, gathered)], ag_send.at[it]).wait()
        whole(rs_send.at[it, pl.ds(0, gathered)], rs_ssem.at[it]).wait()
        whole(ar.at[it, pl.ds(0, 2 * chips - 1)], ar_ssem.at[it]).wait()


def per_device(sizes, features, labels, start_weights, hist_s, hist_y):
    ny, nx, nz = sizes
    chips = ny * nx * nz
    m = hist_s.shape[0]
    x = features.reshape(2, 8, chips, 2, 16, 128).transpose(0, 2, 3, 4, 1, 5)
    x = x.reshape(2, chips, 2, 128, 128)
    vmem = pl.BlockSpec(memory_space=pltpu.VMEM)
    hbm = pl.BlockSpec(memory_space=pl.ANY)
    dma = pltpu.SemaphoreType.DMA
    own = jax.ShapeDtypeStruct((16, 128), F32)
    new, direction = pl.pallas_call(
        functools.partial(kernel, sizes),
        out_shape=(own, own),
        in_specs=[hbm, pl.BlockSpec(memory_space=pltpu.SMEM), vmem, hbm, hbm],
        out_specs=(vmem, vmem),
        scratch_shapes=[
            pltpu.VMEM((chips, 4, 128, 128), BF16),
            pltpu.VMEM((m, 2048), F32),
            pltpu.VMEM((m, 2048), F32),
            pltpu.VMEM((ITERS, chips, 16, 128), BF16),
            pltpu.VMEM((ITERS, chips, 16, 128), BF16),
            pltpu.VMEM((ITERS, chips, 16, 128), BF16),
            pltpu.VMEM((ITERS, 2 * chips, 1, 128), F32),
            pltpu.VMEM((24, 128), F32),
            pltpu.VMEM((24, 128), F32),
            pltpu.VMEM((2, 24, 128), F32),
            pltpu.VMEM((3, 4, 24, 128), F32),
            pltpu.VMEM((8, 128), F32),
            pltpu.VMEM((8, 128), F32),
            pltpu.VMEM((ITERS, 8, 128), F32),
            pltpu.VMEM((ITERS, 8, 128), F32),
            pltpu.VMEM((16, 512), BF16),
            pltpu.VMEM((128, 128), F32),
            pltpu.VMEM((128, 128), F32),
            pltpu.VMEM((16, 128), F32),
            pltpu.VMEM((16, 128), F32),
            pltpu.VMEM((16, 128), F32),
            dma((2,)), dma((2,)), dma((2,)), dma((2,)),
            dma((ITERS,)), dma((ITERS,)), dma((ITERS,)), dma((ITERS,)),
            dma((ITERS,)), dma((ITERS,)),
            dma((4, 3)), dma((4, 3)), dma((2,)), dma((ITERS,)), dma((ITERS,)),
        ],
        compiler_params=pltpu.CompilerParams(collective_id=0, has_side_effects=True),
    )(x, labels, start_weights.reshape(16, 128), hist_s, hist_y)
    return new.reshape(2048), direction.reshape(2048)


def solution(mesh):
    ny, rest = mesh.shape["ex"], mesh.shape["ft"] // 2
    nx = round(rest ** 0.5)
    sizes = (ny, nx, rest // nx)
    return jax.shard_map(
        functools.partial(per_device, sizes),
        mesh=mesh,
        in_specs=(
            P(("ex", "ft"), None),
            P(("ex", "ft")),
            P(("ex", "ft")),
            P(None, ("ex", "ft")),
            P(None, ("ex", "ft")),
        ),
        out_specs=(P(("ex", "ft")), P(("ex", "ft"))),
        check_vma=False,
    )
```

```python
import functools
import itertools

import jax
import jax.numpy as jnp
from jax import lax
from jax.experimental import pallas as pl
from jax.experimental.pallas import tpu as pltpu
from jax.sharding import PartitionSpec as P

ITERS = 2
MESH = pl.DeviceIdType.MESH
HI = lax.Precision.HIGHEST
F32 = jnp.float32
BF16 = jnp.bfloat16
BATCHES = (8, 8, 16, 16, 16)


def contract_last(a, b):
    return lax.dot_general(a, b, (((1,), (1,)), ((), ())), precision=HI, preferred_element_type=F32)


def hops(offset, sizes):
    return sum(min(o, n - o) for o, n in zip(offset, sizes))


def kernel(
    sizes, x_hbm, lab_hbm, w_hbm, s_hbm, y_hbm, out_ref,
    x_v, x_out, lab_ref, w_ref, s_v, y_v, w_own, wg, rs_send, rs_recv, ar_own, ar, gl, gtmp, gcore, gax,
    lab_send, lab_recv, m_send, m_recv, r_ref, acc_ref, t_ref, g_ref, gp_ref, d_ref,
    x_sem, xr_send, xr_recv, h_sem, ag_send, ag_recv, rs_ssem, rs_rsem,
    ar_ssem, ar_rsem, g_ssem, g_rsem, l_sem, m_ssem, m_rsem,
):
    ny, nx, nz = sizes
    plane = nx * nz
    chips = ny * plane
    m = s_v.shape[0]
    ex = lax.axis_index("ex")
    ft = lax.axis_index("ft")
    core = lax.rem(ft, 2)
    xz = ft // 2
    px, pz = xz // nz, lax.rem(xz, nz)
    chip = ex * plane + xz
    other = 1 - core
    partner = (ex, xz * 2 + other)

    steps = (plane, nz, 1)
    mine = (ex, px, pz)
    ahead = [[lax.rem(p + o, n) * d for o in range(n)] for p, n, d in zip(mine, sizes, steps)]
    behind = [[lax.rem(p + n - o, n) * d for o in range(n)] for p, n, d in zip(mine, sizes, steps)]

    def index(offset, table):
        return table[0][offset[0]] + table[1][offset[1]] + table[2][offset[2]]

    at_y = [lax.rem(ex + o, ny) for o in range(ny)]

    def peer(offset):
        return at_y[offset[0]], ahead[1][offset[1]] + ahead[2][offset[2]]

    def dest(place):
        return (place[0], place[1] * 2 + other)

    offsets = sorted(
        itertools.product(*map(range, sizes)),
        key=lambda o: -hops(o, sizes))
    rounds = chips // 8

    def round_of(offset):
        j = 0
        for o, n in zip(offset, sizes):
            j = 2 * j + (1 if n == 4 and o in (3, 0) else 0)
        return {3: 4, 4: 3}.get(j, j)

    def round_blocks(k, table):
        j = k + jnp.where(k == 3, 1, 0) - jnp.where(k == 4, 1, 0)
        lows = []
        for places, high in zip(table, (j // 4, lax.rem(j // 2, 2), lax.rem(j, 2))):
            if len(places) == 4:
                lows.append([jnp.where(high == 0, places[2], places[3]), jnp.where(high == 0, places[1], places[0])])
            else:
                lows.append([places[1], places[0]])
        return [a + b + c for a in lows[0] for b in lows[1] for c in lows[2]]

    hist = [
        pltpu.make_async_copy(s_hbm, s_v, h_sem.at[0]),
        pltpu.make_async_copy(y_hbm, y_v, h_sem.at[1]),
    ]
    small = [
        pltpu.make_async_copy(w_hbm, w_ref, h_sem.at[2]),
        pltpu.make_async_copy(lab_hbm, lab_ref, h_sem.at[3]),
    ]
    for copy in small + hist:
        copy.start()
    local = []
    for h in range(2):
        copy = pltpu.make_async_copy(x_hbm.at[h, :, other], x_v.at[:, h], x_sem.at[h])
        copy.start()
        local.append(copy)
    staged = []
    for h in range(2):
        copy = pltpu.make_async_copy(x_hbm.at[h, :, core], x_out.at[:, h], x_sem.at[2 + h])
        copy.start()
        staged.append(copy)

    barrier = pltpu.get_barrier_semaphore()
    for offset in offsets:
        pl.semaphore_signal(barrier, inc=1, device_id=dest(peer(offset)), device_id_type=MESH)

    row8 = lax.broadcasted_iota(jnp.int32, (8, 128), 0)
    lanes8 = lax.broadcasted_iota(jnp.int32, (8, 128), 1)
    for copy in small:
        copy.wait()
    lab = jnp.zeros((8, 128), F32)
    for h in range(2):
        for e in range(8):
            value = lab_ref[h * 8 + e].astype(F32)
            lab = jnp.where((row8 == e) & (lanes8 // 32 == h), value, lab)
    lab_send[...] = lab
    w_own[0] = w_ref[...].astype(BF16)
    acc_ref[...] = jnp.zeros_like(acc_ref)
    t_ref[...] = jnp.zeros_like(t_ref)
    gl[...] = jnp.zeros_like(gl)
    gtmp[...] = jnp.zeros_like(gtmp)
    for copy in hist:
        copy.wait()
    gl[0:m, 0:m] = contract_last(s_v[...], y_v[...])
    gtmp[0:m, 0:m] = contract_last(y_v[...], y_v[...])
    gcore[core] = gl[...] + pltpu.roll(gtmp[...], 64, 1)
    pl.semaphore_wait(barrier, chips)

    def whole(ref, sem):
        return pltpu.make_async_copy(ref, ref, sem)

    def gather_start(it):
        for offset in offsets:
            pltpu.make_async_remote_copy(
                src_ref=w_own.at[it], dst_ref=wg.at[it, chip],
                send_sem=ag_send.at[it], recv_sem=ag_recv.at[it, round_of(offset)],
                device_id=dest(peer(offset)), device_id_type=MESH).start()

    gather_start(0)

    def gram_send(stage):
        copies = []
        if stage == 3:
            copies.append(pltpu.make_async_remote_copy(
                src_ref=gcore.at[core], dst_ref=gcore.at[core],
                send_sem=g_ssem.at[3, 0], recv_sem=g_rsem.at[3, 0],
                device_id=partner, device_id_type=MESH))
        else:
            own = mine[stage]
            for off in range(1, sizes[stage]):
                offset = tuple(off if a == stage else 0 for a in range(3))
                copies.append(pltpu.make_async_remote_copy(
                    src_ref=gax.at[stage, own], dst_ref=gax.at[stage, own],
                    send_sem=g_ssem.at[stage, off - 1], recv_sem=g_rsem.at[stage, off - 1],
                    device_id=dest(peer(offset)), device_id_type=MESH))
        for copy in copies:
            copy.start()
        return copies

    def gram_sum(stage, copies):
        for copy in copies:
            copy.wait()
        if stage == 3:
            return gcore[0] + gcore[1]
        total = gax[stage, 0]
        for place in range(1, sizes[stage]):
            total = total + gax[stage, place]
        return total

    gram = gram_send(3)
    for copy in staged:
        copy.wait()
    for offset in reversed(offsets):
        c = index(offset, behind)
        pltpu.make_async_remote_copy(
            src_ref=x_out.at[c], dst_ref=x_v.at[c, 2:4],
            send_sem=xr_send.at[0], recv_sem=xr_recv.at[round_of(offset)],
            device_id=partner, device_id_type=MESH).start()
    lab_copy = pltpu.make_async_remote_copy(
        src_ref=lab_send, dst_ref=lab_recv, send_sem=l_sem.at[0], recv_sem=l_sem.at[1],
        device_id=partner, device_id_type=MESH)
    lab_copy.start()

    gax[0, ex] = gram_sum(3, gram)
    gram = gram_send(0)

    row16 = lax.broadcasted_iota(jnp.int32, (16, 128), 0)
    tile16 = lax.broadcasted_iota(jnp.int32, (16, 128), 1) // 8
    on_diag = row16 == tile16
    row24 = lax.broadcasted_iota(jnp.int32, (24, 128), 0)
    lane24 = lax.broadcasted_iota(jnp.int32, (24, 128), 1)
    lane1 = lax.broadcasted_iota(jnp.int32, (1, 128), 1)
    eye = jnp.where((row24 == lane24) & (row24 < m), 1.0, 0.0).astype(F32)
    turn = jnp.where(lax.rem(lanes8, 8) == row8, 1.0, 0.0).astype(F32)

    def margin_terms(it, blocks, accs):
        accs = list(accs)
        left = jnp.concatenate([wg[it, c] for c in blocks], axis=1)
        right = jnp.concatenate([x_v[c, 3] for c in blocks], axis=1)
        accs[6] = accs[6] + lax.dot_general(
            left, right, (((1,), (1,)), ((), ())), preferred_element_type=F32)
        for c in blocks:
            for t in range(0, 16, 2):
                w = wg[it, c, t:t + 2, :].astype(F32)
                w = jnp.concatenate(
                    [jnp.broadcast_to(w[0:1], (8, 128)), jnp.broadcast_to(w[1:2], (8, 128))], axis=0)
                for f in range(3):
                    prod = x_v[c, f, t * 8:t * 8 + 16, :].astype(F32) * w
                    accs[f] = accs[f] + prod[0:8]
                    accs[3 + f] = accs[3 + f] + prod[8:16]
        return tuple(accs)

    def zeros(count):
        return tuple(jnp.zeros((8, 128), F32) for _ in range(count))

    def lane_sums(accs):
        return [jnp.sum(acc, axis=1, keepdims=True) for acc in accs]

    def spread_halves(cols):
        out = jnp.broadcast_to(cols[0], (8, 128))
        for k in range(1, 4):
            out = jnp.where(lanes8 // 32 == k, cols[k], out)
        return out

    weights = w_ref[...]
    rinv = rinvt = yy = diag = gamma0 = None
    for it in range(ITERS):
        if it == 0:
            for copy in local:
                copy.wait()

        def arrive(i, accs):
            k = rounds - 1 - i
            if it == 0:
                whole(x_out.at[pl.ds(0, 8)], xr_recv.at[k]).wait()
            whole(wg.at[it, pl.ds(0, 8)], ag_recv.at[it, k]).wait()
            return margin_terms(it, round_blocks(k, behind), accs)

        accs = lax.fori_loop(0, rounds, arrive, zeros(6) + (jnp.zeros((16, 128), F32),))
        line = jnp.sum(jnp.where(on_diag, accs[6], 0.0), axis=0, keepdims=True)
        cols = lane_sums([accs[f] + accs[3 + f] for f in range(3)] + [turn * line])
        m_send[it] = spread_halves(cols)
        m_copy = pltpu.make_async_remote_copy(
            src_ref=m_send.at[it], dst_ref=m_recv.at[it],
            send_sem=m_ssem.at[it], recv_sem=m_rsem.at[it],
            device_id=partner, device_id_type=MESH)
        m_copy.start()
        if it == 0:
            lab_copy.wait()
            lab_all = lab_send[...] + pltpu.roll(lab_recv[...], 64, 1)
            gax[1, px] = gram_sum(0, gram)
            gram = gram_send(1)
        m_copy.wait()
        margin = m_send[it] + pltpu.roll(m_recv[it], 64, 1)
        resid = jax.nn.sigmoid(margin) - lab_all
        for k in range(4):
            line = jnp.sum(turn * resid[:, k * 32:k * 32 + 1], axis=0, keepdims=True)
            r_ref[:, k * 128:(k + 1) * 128] = jnp.where(on_diag, line, 0.0).astype(BF16)

        def scatter_send(batch):
            for offset in batch:
                pltpu.make_async_remote_copy(
                    src_ref=rs_send.at[it, index(offset, ahead)], dst_ref=rs_recv.at[it, chip],
                    send_sem=rs_ssem.at[it], recv_sem=rs_rsem.at[it],
                    device_id=dest(peer(offset)), device_id_type=MESH).start()

        lines = r_ref[...]
        start = 0
        for size in BATCHES:
            batch = offsets[start:min(start + size, chips)]
            start += size
            for j in range(0, len(batch), 2):
                c0, c1 = index(batch[j], ahead), index(batch[j + 1], ahead)
                both = jnp.concatenate([x_v[c0].reshape(512, 128), x_v[c1].reshape(512, 128)], axis=1)
                term = jnp.dot(lines, both, preferred_element_type=F32).astype(BF16)
                rs_send[it, c0] = term[:, 0:128]
                rs_send[it, c1] = term[:, 128:256]
            scatter_send(batch)
        if it == 0:
            gax[2, pz] = gram_sum(1, gram)
            gram = gram_send(2)
            total = gram_sum(2, gram)
            upper = jnp.where((row24 <= lane24) & (lane24 < m), total, 0.0)
            yy = jnp.where((lane24 < m) & (row24 < m), pltpu.roll(total, 64, 1), 0.0)
            diag = upper * eye
            inv = eye
            for i in reversed(range(m)):
                line = inv[i:i + 1, :] / upper[i:i + 1, i:i + 1]
                column = jnp.where(row24[:, 0:1] < i, upper[:, i:i + 1], 0.0)
                inv = jnp.where(row24 == i, line, inv - column * line)
            rinv = inv
            t_ref[0:24, :] = inv
            rinvt = t_ref[...].T[0:24, :]
            gamma0 = upper[m - 1:m, m - 1:m] / yy[m - 1:m, m - 1:m]
        whole(rs_recv.at[it], rs_rsem.at[it]).wait()

        def add(k, total):
            return total + rs_recv[it, k].astype(F32)
        grad = lax.fori_loop(0, chips, add, jnp.zeros((16, 128), F32), unroll=8) + 0.1 * weights
        g_ref[...] = grad
        vectors = [g_ref]
        if it > 0:
            gp_ref[...] = grad - gp_ref[...]
            vectors.append(gp_ref)
            for t in range(16):
                y_v[0:1, t * 128:(t + 1) * 128] = gp_ref[t:t + 1, :]
        for v, vec in enumerate(vectors):
            acc_s = jnp.zeros((m, 128), F32)
            acc_y = jnp.zeros((m, 128), F32)
            for t in range(16):
                line = vec[t:t + 1, :]
                acc_s = acc_s + s_v[:, t * 128:(t + 1) * 128] * line
                acc_y = acc_y + y_v[:, t * 128:(t + 1) * 128] * line
            acc_ref[v * 64:v * 64 + m, :] = acc_s
            acc_ref[v * 64 + 32:v * 64 + 32 + m, :] = acc_y
        sums = contract_last(jnp.ones((8, 128), F32), acc_ref[...])
        ar_own[it] = sums[0:1, :]
        ar[it, chip * 2 + core] = sums[0:1, :]

        def total_send(device):
            pltpu.make_async_remote_copy(
                src_ref=ar_own.at[it], dst_ref=ar.at[it, chip * 2 + core],
                send_sem=ar_ssem.at[it], recv_sem=ar_rsem.at[it],
                device_id=device, device_id_type=MESH).start()

        for offset in offsets[:-1]:
            cy, cxz = peer(offset)
            total_send((cy, cxz * 2))
            total_send((cy, cxz * 2 + 1))
        total_send(partner)
        whole(ar.at[it, pl.ds(0, 2 * chips - 1)], ar_rsem.at[it]).wait()
        tot = jnp.broadcast_to(jnp.sum(ar[it], axis=0), (8, 128))
        u, hh = tot[0:1], pltpu.roll(tot, 96, 1)[0:1]
        if it == 0:
            gamma = gamma0
            alpha = -jnp.sum(rinv * u, axis=1, keepdims=True)
            p = gamma * (jnp.sum(yy * alpha, axis=0, keepdims=True) + hh)
            p = p + jnp.sum(diag * alpha, axis=0, keepdims=True)
            coef = jnp.sum(rinvt * p, axis=1, keepdims=True)
        else:
            v, z = pltpu.roll(tot, 64, 1)[0:1], pltpu.roll(tot, 32, 1)[0:1]
            v0, z0, u0 = v[:, 0:1], z[:, 0:1], u[:, 0:1]
            gamma = v0 / z0
            a0 = -u0 / v0
            old = (row24 > 0) & (lane24 > 0)
            rm, rmt = jnp.where(old, rinv, 0.0), jnp.where(old, rinvt, 0.0)
            ru = jnp.sum(rm * u, axis=1, keepdims=True)
            rv = jnp.sum(rm * v, axis=1, keepdims=True)
            rv_flat = jnp.sum(eye * rv, axis=0, keepdims=True)
            alpha = jnp.where(row24[:, 0:1] == 0, a0, -(ru + rv * a0))
            flat = jnp.sum(eye * alpha, axis=0, keepdims=True)
            newest = jnp.sum(jnp.where(lane1 < m, z, 0.0) * flat, axis=1, keepdims=True)
            q = jnp.sum(jnp.where(old, yy, 0.0) * alpha, axis=0, keepdims=True) + z * a0
            p = gamma * (q + hh) + jnp.sum(diag * alpha, axis=0, keepdims=True)
            coef = jnp.sum(rmt * p, axis=1, keepdims=True)
            rest = jnp.sum(rv_flat * p, axis=1, keepdims=True)
            c0 = (gamma * (newest + hh[:, 0:1]) + v0 * a0 - rest) / v0
            coef = jnp.where(row24[:, 0:1] == 0, c0, coef)
        cs, cy = coef[0:m], (-gamma * alpha)[0:m]
        for t in range(16):
            cols = slice(t * 128, (t + 1) * 128)
            d_ref[t:t + 1, :] = jnp.sum(cs * s_v[:, cols] + cy * y_v[:, cols], axis=0, keepdims=True)
        direction = d_ref[...] - gamma * g_ref[...]
        new = weights + direction
        if it < ITERS - 1:
            w_own[it + 1] = new.astype(BF16)
            gather_start(it + 1)
            gp_ref[...] = grad
            d_ref[...] = new - weights
            for t in range(16):
                s_v[0:1, t * 128:(t + 1) * 128] = d_ref[t:t + 1, :]
            weights = new
        else:
            out_ref[0] = new
            out_ref[1] = direction

    whole(x_out, xr_send.at[0]).wait()
    for it in range(ITERS):
        whole(wg.at[it], ag_send.at[it]).wait()
        whole(rs_send.at[it], rs_ssem.at[it]).wait()
        whole(ar.at[it, pl.ds(0, 2 * chips - 1)], ar_ssem.at[it]).wait()


def per_device(sizes, features, labels, start_weights, hist_s, hist_y):
    ny, nx, nz = sizes
    chips = ny * nx * nz
    m = hist_s.shape[0]
    x = features.reshape(2, 8, chips, 2, 16, 128).transpose(0, 2, 3, 4, 1, 5)
    x = x.reshape(2, chips, 2, 128, 128)
    vmem = pl.BlockSpec(memory_space=pltpu.VMEM)
    hbm = pl.BlockSpec(memory_space=pl.ANY)
    dma = pltpu.SemaphoreType.DMA
    out = pl.pallas_call(
        functools.partial(kernel, sizes),
        out_shape=pltpu.VMEM((2, 16, 128), F32),
        in_specs=[hbm] * 5,
        out_specs=vmem,
        scratch_shapes=[
            pltpu.VMEM((chips, 4, 128, 128), BF16),
            pltpu.VMEM((chips, 2, 128, 128), BF16),
            pltpu.SMEM((16,), jnp.int32),
            pltpu.VMEM((16, 128), F32),
            pltpu.VMEM((m, 2048), F32),
            pltpu.VMEM((m, 2048), F32),
            pltpu.VMEM((ITERS, 16, 128), BF16),
            pltpu.VMEM((ITERS, chips, 16, 128), BF16),
            pltpu.VMEM((ITERS, chips, 16, 128), BF16),
            pltpu.VMEM((ITERS, chips, 16, 128), BF16),
            pltpu.VMEM((ITERS, 1, 128), F32),
            pltpu.VMEM((ITERS, 2 * chips, 1, 128), F32),
            pltpu.VMEM((24, 128), F32),
            pltpu.VMEM((24, 128), F32),
            pltpu.VMEM((2, 24, 128), F32),
            pltpu.VMEM((3, 4, 24, 128), F32),
            pltpu.VMEM((8, 128), F32),
            pltpu.VMEM((8, 128), F32),
            pltpu.VMEM((ITERS, 8, 128), F32),
            pltpu.VMEM((ITERS, 8, 128), F32),
            pltpu.VMEM((16, 512), BF16),
            pltpu.VMEM((128, 128), F32),
            pltpu.VMEM((128, 128), F32),
            pltpu.VMEM((16, 128), F32),
            pltpu.VMEM((16, 128), F32),
            pltpu.VMEM((16, 128), F32),
            dma((4,)), dma((1,)), dma((chips // 8,)), dma((4,)),
            dma((ITERS,)), dma((ITERS, chips // 8)), dma((ITERS,)), dma((ITERS,)),
            dma((ITERS,)), dma((ITERS,)),
            dma((4, 3)), dma((4, 3)), dma((2,)), dma((ITERS,)), dma((ITERS,)),
        ],
        compiler_params=pltpu.CompilerParams(collective_id=0, has_side_effects=True),
    )(x, labels, start_weights.reshape(16, 128), hist_s, hist_y)
    out = out.reshape(2, 2048)
    return out[0], out[1]


def solution(mesh):
    ny, rest = mesh.shape["ex"], mesh.shape["ft"] // 2
    nx = round(rest ** 0.5)
    sizes = (ny, nx, rest // nx)
    return jax.shard_map(
        functools.partial(per_device, sizes),
        mesh=mesh,
        in_specs=(
            P(("ex", "ft"), None),
            P(("ex", "ft")),
            P(("ex", "ft")),
            P(None, ("ex", "ft")),
            P(None, ("ex", "ft")),
        ),
        out_specs=(P(("ex", "ft")), P(("ex", "ft"))),
        check_vma=False,
    )
```

```python
import functools
import itertools

import jax
import jax.numpy as jnp
from jax import lax
from jax.experimental import pallas as pl
from jax.experimental.pallas import tpu as pltpu
from jax.sharding import PartitionSpec as P

ITERS = 2
MESH = pl.DeviceIdType.MESH
HI = lax.Precision.HIGHEST
F32 = jnp.float32
BF16 = jnp.bfloat16
BATCHES = (8, 8, 16, 16, 16)


def contract_last(a, b):
    return lax.dot_general(a, b, (((1,), (1,)), ((), ())), precision=HI, preferred_element_type=F32)


def hops(offset, sizes):
    return sum(min(o, n - o) for o, n in zip(offset, sizes))


def kernel(
    sizes, x_hbm, lab_hbm, w_hbm, s_hbm, y_hbm, out_ref,
    x_v, x_out, x_f, lab_ref, w_ref, s_v, y_v, w_own, wg, rs_send, rs_recv, ar_own, ar, gl, gtmp, gcore, gax,
    lab_send, lab_recv, m_send, m_recv, r_ref, t_ref, g_ref, gp_ref, d_ref,
    x_sem, xr_send, xr_recv, h_sem, ag_send, ag_recv, rs_ssem, rs_rsem,
    ar_ssem, ar_rsem, g_ssem, g_rsem, l_sem, m_ssem, m_rsem,
):
    ny, nx, nz = sizes
    plane = nx * nz
    chips = ny * plane
    m = s_v.shape[0]
    ex = lax.axis_index("ex")
    ft = lax.axis_index("ft")
    core = lax.rem(ft, 2)
    xz = ft // 2
    px, pz = xz // nz, lax.rem(xz, nz)
    chip = ex * plane + xz
    other = 1 - core
    partner = (ex, xz * 2 + other)

    steps = (plane, nz, 1)
    mine = (ex, px, pz)
    ahead = [[lax.rem(p + o, n) * d for o in range(n)] for p, n, d in zip(mine, sizes, steps)]
    behind = [[lax.rem(p + n - o, n) * d for o in range(n)] for p, n, d in zip(mine, sizes, steps)]

    def index(offset, table):
        return table[0][offset[0]] + table[1][offset[1]] + table[2][offset[2]]

    at_y = [lax.rem(ex + o, ny) for o in range(ny)]

    def peer(offset):
        return at_y[offset[0]], ahead[1][offset[1]] + ahead[2][offset[2]]

    def dest(place):
        return (place[0], place[1] * 2 + other)

    offsets = sorted(
        itertools.product(*map(range, sizes)),
        key=lambda o: -hops(o, sizes))
    rounds = chips // 8

    def round_of(offset):
        j = 0
        for o, n in zip(offset, sizes):
            j = 2 * j + (1 if n == 4 and o in (3, 0) else 0)
        return {3: 4, 4: 3}.get(j, j)

    def round_blocks(k, table):
        j = k + jnp.where(k == 3, 1, 0) - jnp.where(k == 4, 1, 0)
        lows = []
        for places, high in zip(table, (j // 4, lax.rem(j // 2, 2), lax.rem(j, 2))):
            if len(places) == 4:
                lows.append([jnp.where(high == 0, places[2], places[3]), jnp.where(high == 0, places[1], places[0])])
            else:
                lows.append([places[1], places[0]])
        return [a + b + c for a in lows[0] for b in lows[1] for c in lows[2]]

    hist = [
        pltpu.make_async_copy(s_hbm, s_v, h_sem.at[0]),
        pltpu.make_async_copy(y_hbm, y_v, h_sem.at[1]),
    ]
    small = [
        pltpu.make_async_copy(w_hbm, w_ref, h_sem.at[2]),
        pltpu.make_async_copy(lab_hbm, lab_ref, h_sem.at[3]),
    ]
    for copy in small + hist:
        copy.start()
    local = []
    for h in range(2):
        copy = pltpu.make_async_copy(x_hbm.at[h, :, other], x_v.at[:, h], x_sem.at[h])
        copy.start()
        local.append(copy)
    staged = []
    for h in range(2):
        copy = pltpu.make_async_copy(x_hbm.at[h, :, core], x_out.at[:, h], x_sem.at[2 + h])
        copy.start()
        staged.append(copy)

    barrier = pltpu.get_barrier_semaphore()
    for offset in offsets:
        pl.semaphore_signal(barrier, inc=1, device_id=dest(peer(offset)), device_id_type=MESH)

    row8 = lax.broadcasted_iota(jnp.int32, (8, 128), 0)
    lanes8 = lax.broadcasted_iota(jnp.int32, (8, 128), 1)
    for copy in small:
        copy.wait()
    lab = jnp.zeros((8, 128), F32)
    for h in range(2):
        for e in range(8):
            value = lab_ref[h * 8 + e].astype(F32)
            lab = jnp.where((row8 == e), value, lab)
        lab_send[h] = lab
    w_own[0] = w_ref[...].astype(BF16)
    t_ref[...] = jnp.zeros_like(t_ref)
    gl[...] = jnp.zeros_like(gl)
    gtmp[...] = jnp.zeros_like(gtmp)
    for copy in hist:
        copy.wait()
    gl[0:m, 0:m] = contract_last(s_v[...], y_v[...])
    gtmp[0:m, 0:m] = contract_last(y_v[...], y_v[...])
    gcore[core] = gl[...] + pltpu.roll(gtmp[...], 64, 1)
    pl.semaphore_wait(barrier, chips)

    def whole(ref, sem):
        return pltpu.make_async_copy(ref, ref, sem)

    def gather_start(it):
        for offset in offsets:
            pltpu.make_async_remote_copy(
                src_ref=w_own.at[it], dst_ref=wg.at[it, chip],
                send_sem=ag_send.at[it], recv_sem=ag_recv.at[it, round_of(offset)],
                device_id=dest(peer(offset)), device_id_type=MESH).start()

    gather_start(0)

    def gram_send(stage):
        copies = []
        if stage == 3:
            copies.append(pltpu.make_async_remote_copy(
                src_ref=gcore.at[core], dst_ref=gcore.at[core],
                send_sem=g_ssem.at[3, 0], recv_sem=g_rsem.at[3, 0],
                device_id=partner, device_id_type=MESH))
        else:
            own = mine[stage]
            for off in range(1, sizes[stage]):
                offset = tuple(off if a == stage else 0 for a in range(3))
                copies.append(pltpu.make_async_remote_copy(
                    src_ref=gax.at[stage, own], dst_ref=gax.at[stage, own],
                    send_sem=g_ssem.at[stage, off - 1], recv_sem=g_rsem.at[stage, off - 1],
                    device_id=dest(peer(offset)), device_id_type=MESH))
        for copy in copies:
            copy.start()
        return copies

    def gram_sum(stage, copies):
        for copy in copies:
            copy.wait()
        if stage == 3:
            return gcore[0] + gcore[1]
        total = gax[stage, 0]
        for place in range(1, sizes[stage]):
            total = total + gax[stage, place]
        return total

    gram = gram_send(3)
    for copy in staged:
        copy.wait()
    for offset in reversed(offsets):
        c = index(offset, behind)
        pltpu.make_async_remote_copy(
            src_ref=x_out.at[c], dst_ref=x_v.at[c, 2:4],
            send_sem=xr_send.at[0], recv_sem=xr_recv.at[round_of(offset)],
            device_id=partner, device_id_type=MESH).start()
    lab_copy = pltpu.make_async_remote_copy(
        src_ref=lab_send, dst_ref=lab_recv, send_sem=l_sem.at[0], recv_sem=l_sem.at[1],
        device_id=partner, device_id_type=MESH)
    lab_copy.start()

    gax[0, ex] = gram_sum(3, gram)
    gram = gram_send(0)

    row16 = lax.broadcasted_iota(jnp.int32, (16, 128), 0)
    tile16 = lax.broadcasted_iota(jnp.int32, (16, 128), 1) // 8
    on_diag = row16 == tile16
    row24 = lax.broadcasted_iota(jnp.int32, (24, 128), 0)
    lane24 = lax.broadcasted_iota(jnp.int32, (24, 128), 1)
    row_m, lane_m = row24[0:m], lane24[0:m]
    lane1 = lax.broadcasted_iota(jnp.int32, (1, 128), 1)
    eye = jnp.where((row24 == lane24) & (row24 < m), 1.0, 0.0).astype(F32)
    turn = jnp.where(lax.rem(lanes8, 8) == row8, 1.0, 0.0).astype(F32)

    def margin_terms(it, blocks, accs):
        accs = list(accs)
        count = 3 if it == 0 else 4
        if it == 0:
            left = jnp.concatenate([wg[it, c] for c in blocks], axis=1)
            right = jnp.concatenate([x_v[c, 3] for c in blocks], axis=1)
            accs[6] = accs[6] + lax.dot_general(
                left, right, (((1,), (1,)), ((), ())), preferred_element_type=F32)
        for c in blocks:
            for t in range(0, 16, 2):
                w = wg[it, c, t:t + 2, :].astype(F32)
                w = jnp.concatenate(
                    [jnp.broadcast_to(w[0:1], (8, 128)), jnp.broadcast_to(w[1:2], (8, 128))], axis=0)
                for f in range(count):
                    if it == 0:
                        prod = x_v[c, f, t * 8:t * 8 + 16, :].astype(F32) * w
                    else:
                        prod = x_f[c, f, t * 8:t * 8 + 16, :] * w
                    accs[f] = accs[f] + prod[0:8]
                    accs[count + f] = accs[count + f] + prod[8:16]
        return tuple(accs)

    def zeros(count):
        return tuple(jnp.zeros((8, 128), F32) for _ in range(count))

    def lane_sums(accs):
        return [jnp.sum(acc, axis=1, keepdims=True) for acc in accs]

    weights = w_ref[...]
    rinv = rinvt = yy = diag = gamma0 = None
    for it in range(ITERS):
        if it == 0:
            for copy in local:
                copy.wait()

        def arrive(i, accs):
            k = rounds - 1 - i
            if it == 0:
                whole(x_out.at[pl.ds(0, 8)], xr_recv.at[k]).wait()
            whole(wg.at[it, pl.ds(0, 8)], ag_recv.at[it, k]).wait()
            return margin_terms(it, round_blocks(k, behind), accs)

        if it == 0:
            accs = lax.fori_loop(0, rounds, arrive, zeros(6) + (jnp.zeros((16, 128), F32),))
            line = jnp.sum(jnp.where(on_diag, accs[6], 0.0), axis=0, keepdims=True)
            cols = lane_sums([accs[f] + accs[3 + f] for f in range(3)] + [turn * line])
        else:
            accs = lax.fori_loop(0, rounds, arrive, zeros(8))
            cols = lane_sums([accs[f] + accs[4 + f] for f in range(4)])
        for k in range(4):
            m_send[it, (k + 2) % 4] = jnp.broadcast_to(cols[k], (8, 128))
        m_copy = pltpu.make_async_remote_copy(
            src_ref=m_send.at[it], dst_ref=m_recv.at[it],
            send_sem=m_ssem.at[it], recv_sem=m_rsem.at[it],
            device_id=partner, device_id_type=MESH)
        m_copy.start()
        if it == 0:
            lab_copy.wait()
            lab_all = [lab_send[0], lab_send[1], lab_recv[0], lab_recv[1]]
            gax[1, px] = gram_sum(0, gram)
            gram = gram_send(1)
        m_copy.wait()
        for k in range(4):
            resid = jax.nn.sigmoid(m_send[it, (k + 2) % 4] + m_recv[it, k]) - lab_all[k]
            line = jnp.sum(turn * resid, axis=0, keepdims=True)
            r_ref[:, k * 128:(k + 1) * 128] = jnp.where(on_diag, line, 0.0).astype(BF16)

        def scatter_send(batch):
            for offset in batch:
                pltpu.make_async_remote_copy(
                    src_ref=rs_send.at[it, index(offset, ahead)], dst_ref=rs_recv.at[it, chip],
                    send_sem=rs_ssem.at[it], recv_sem=rs_rsem.at[it],
                    device_id=dest(peer(offset)), device_id_type=MESH).start()

        lines = r_ref[...]
        start = 0
        for size in BATCHES:
            batch = offsets[start:min(start + size, chips)]
            start += size
            for j in range(0, len(batch), 2):
                c0, c1 = index(batch[j], ahead), index(batch[j + 1], ahead)
                both = jnp.concatenate([x_v[c0].reshape(512, 128), x_v[c1].reshape(512, 128)], axis=1)
                term = jnp.dot(lines, both, preferred_element_type=F32).astype(BF16)
                rs_send[it, c0] = term[:, 0:128]
                rs_send[it, c1] = term[:, 128:256]
            scatter_send(batch)
        if it == 0:
            gax[2, pz] = gram_sum(1, gram)
            gram = gram_send(2)
            total = gram_sum(2, gram)
            upper = jnp.where((row24 <= lane24) & (lane24 < m), total, 0.0)
            yy = jnp.where((lane24 < m) & (row24 < m), pltpu.roll(total, 64, 1), 0.0)
            diag = upper * eye
            inv = eye
            for i in reversed(range(m)):
                line = inv[i:i + 1, :] / upper[i:i + 1, i:i + 1]
                column = jnp.where(row24[:, 0:1] < i, upper[:, i:i + 1], 0.0)
                inv = jnp.where(row24 == i, line, inv - column * line)
            rinv = inv
            t_ref[0:24, :] = inv
            rinvt = t_ref[...].T[0:24, :]
            gamma0 = upper[m - 1:m, m - 1:m] / yy[m - 1:m, m - 1:m]
        whole(rs_recv.at[it], rs_rsem.at[it]).wait()

        def add(k, total):
            return total + rs_recv[it, k].astype(F32)
        grad = lax.fori_loop(0, chips, add, jnp.zeros((16, 128), F32), unroll=8) + 0.1 * weights
        g_ref[...] = grad
        vectors = [g_ref]
        if it > 0:
            gp_ref[...] = grad - gp_ref[...]
            vectors.append(gp_ref)
            for t in range(16):
                y_v[0:1, t * 128:(t + 1) * 128] = gp_ref[t:t + 1, :]
        sums = jnp.zeros((m, 128), F32)
        for v, vec in enumerate(vectors):
            acc_s = jnp.zeros((m, 128), F32)
            acc_y = jnp.zeros((m, 128), F32)
            for t in range(16):
                line = vec[t:t + 1, :]
                acc_s = acc_s + s_v[:, t * 128:(t + 1) * 128] * line
                acc_y = acc_y + y_v[:, t * 128:(t + 1) * 128] * line
            for part, acc in ((2 * v, acc_s), (2 * v + 1, acc_y)):
                own_lane = lane_m == row_m + 32 * part
                sums = sums + jnp.where(own_lane, jnp.sum(acc, axis=1, keepdims=True), 0.0)
        sums = jnp.sum(sums, axis=0, keepdims=True)
        ar_own[it] = sums
        ar[it, chip * 2 + core] = sums

        def total_send(device):
            pltpu.make_async_remote_copy(
                src_ref=ar_own.at[it], dst_ref=ar.at[it, chip * 2 + core],
                send_sem=ar_ssem.at[it], recv_sem=ar_rsem.at[it],
                device_id=device, device_id_type=MESH).start()

        for offset in offsets[:-1]:
            cy, cxz = peer(offset)
            total_send((cy, cxz * 2))
            total_send((cy, cxz * 2 + 1))
        total_send(partner)
        if it == 0:
            def widen(c, carry):
                x_f[c] = x_v[c].astype(F32)
                return carry
            lax.fori_loop(0, chips, widen, 0)
        whole(ar.at[it, pl.ds(0, 2 * chips - 1)], ar_rsem.at[it]).wait()
        tot = jnp.broadcast_to(jnp.sum(ar[it], axis=0), (8, 128))
        u, hh = tot[0:1], pltpu.roll(tot, 96, 1)[0:1]
        if it == 0:
            gamma = gamma0
            alpha = -jnp.sum(rinv * u, axis=1, keepdims=True)
            p = gamma * (jnp.sum(yy * alpha, axis=0, keepdims=True) + hh)
            p = p + jnp.sum(diag * alpha, axis=0, keepdims=True)
            coef = jnp.sum(rinvt * p, axis=1, keepdims=True)
        else:
            v, z = pltpu.roll(tot, 64, 1)[0:1], pltpu.roll(tot, 32, 1)[0:1]
            v0, z0, u0 = v[:, 0:1], z[:, 0:1], u[:, 0:1]
            gamma = v0 / z0
            a0 = -u0 / v0
            old = (row24 > 0) & (lane24 > 0)
            rm, rmt = jnp.where(old, rinv, 0.0), jnp.where(old, rinvt, 0.0)
            ru = jnp.sum(rm * u, axis=1, keepdims=True)
            rv = jnp.sum(rm * v, axis=1, keepdims=True)
            rv_flat = jnp.sum(eye * rv, axis=0, keepdims=True)
            alpha = jnp.where(row24[:, 0:1] == 0, a0, -(ru + rv * a0))
            flat = jnp.sum(eye * alpha, axis=0, keepdims=True)
            newest = jnp.sum(jnp.where(lane1 < m, z, 0.0) * flat, axis=1, keepdims=True)
            q = jnp.sum(jnp.where(old, yy, 0.0) * alpha, axis=0, keepdims=True) + z * a0
            p = gamma * (q + hh) + jnp.sum(diag * alpha, axis=0, keepdims=True)
            coef = jnp.sum(rmt * p, axis=1, keepdims=True)
            rest = jnp.sum(rv_flat * p, axis=1, keepdims=True)
            c0 = (gamma * (newest + hh[:, 0:1]) + v0 * a0 - rest) / v0
            coef = jnp.where(row24[:, 0:1] == 0, c0, coef)
        cs, cy = coef[0:m], (-gamma * alpha)[0:m]
        for t in range(16):
            cols = slice(t * 128, (t + 1) * 128)
            d_ref[t:t + 1, :] = jnp.sum(cs * s_v[:, cols] + cy * y_v[:, cols], axis=0, keepdims=True)
        direction = d_ref[...] - gamma * g_ref[...]
        new = weights + direction
        if it < ITERS - 1:
            w_own[it + 1] = new.astype(BF16)
            gather_start(it + 1)
            gp_ref[...] = grad
            d_ref[...] = new - weights
            for t in range(16):
                s_v[0:1, t * 128:(t + 1) * 128] = d_ref[t:t + 1, :]
            weights = new
        else:
            out_ref[0] = new
            out_ref[1] = direction

    whole(x_out, xr_send.at[0]).wait()
    for it in range(ITERS):
        whole(wg.at[it], ag_send.at[it]).wait()
        whole(rs_send.at[it], rs_ssem.at[it]).wait()
        whole(ar.at[it, pl.ds(0, 2 * chips - 1)], ar_ssem.at[it]).wait()


def per_device(sizes, features, labels, start_weights, hist_s, hist_y):
    ny, nx, nz = sizes
    chips = ny * nx * nz
    m = hist_s.shape[0]
    x = features.reshape(2, 8, chips, 2, 16, 128).transpose(0, 2, 3, 4, 1, 5)
    x = x.reshape(2, chips, 2, 128, 128)
    vmem = pl.BlockSpec(memory_space=pltpu.VMEM)
    hbm = pl.BlockSpec(memory_space=pl.ANY)
    dma = pltpu.SemaphoreType.DMA
    out = pl.pallas_call(
        functools.partial(kernel, sizes),
        out_shape=pltpu.VMEM((2, 16, 128), F32),
        in_specs=[hbm] * 5,
        out_specs=vmem,
        scratch_shapes=[
            pltpu.VMEM((chips, 4, 128, 128), BF16),
            pltpu.VMEM((chips, 2, 128, 128), BF16),
            pltpu.VMEM((chips, 4, 128, 128), F32),
            pltpu.SMEM((16,), jnp.int32),
            pltpu.VMEM((16, 128), F32),
            pltpu.VMEM((m, 2048), F32),
            pltpu.VMEM((m, 2048), F32),
            pltpu.VMEM((ITERS, 16, 128), BF16),
            pltpu.VMEM((ITERS, chips, 16, 128), BF16),
            pltpu.VMEM((ITERS, chips, 16, 128), BF16),
            pltpu.VMEM((ITERS, chips, 16, 128), BF16),
            pltpu.VMEM((ITERS, 1, 128), F32),
            pltpu.VMEM((ITERS, 2 * chips, 1, 128), F32),
            pltpu.VMEM((24, 128), F32),
            pltpu.VMEM((24, 128), F32),
            pltpu.VMEM((2, 24, 128), F32),
            pltpu.VMEM((3, 4, 24, 128), F32),
            pltpu.VMEM((2, 8, 128), F32),
            pltpu.VMEM((2, 8, 128), F32),
            pltpu.VMEM((ITERS, 4, 8, 128), F32),
            pltpu.VMEM((ITERS, 4, 8, 128), F32),
            pltpu.VMEM((16, 512), BF16),
            pltpu.VMEM((128, 128), F32),
            pltpu.VMEM((16, 128), F32),
            pltpu.VMEM((16, 128), F32),
            pltpu.VMEM((16, 128), F32),
            dma((4,)), dma((1,)), dma((chips // 8,)), dma((4,)),
            dma((ITERS,)), dma((ITERS, chips // 8)), dma((ITERS,)), dma((ITERS,)),
            dma((ITERS,)), dma((ITERS,)),
            dma((4, 3)), dma((4, 3)), dma((2,)), dma((ITERS,)), dma((ITERS,)),
        ],
        compiler_params=pltpu.CompilerParams(collective_id=0, has_side_effects=True),
    )(x, labels, start_weights.reshape(16, 128), hist_s, hist_y)
    out = out.reshape(2, 2048)
    return out[0], out[1]


def solution(mesh):
    ny, rest = mesh.shape["ex"], mesh.shape["ft"] // 2
    nx = round(rest ** 0.5)
    sizes = (ny, nx, rest // nx)
    return jax.shard_map(
        functools.partial(per_device, sizes),
        mesh=mesh,
        in_specs=(
            P(("ex", "ft"), None),
            P(("ex", "ft")),
            P(("ex", "ft")),
            P(None, ("ex", "ft")),
            P(None, ("ex", "ft")),
        ),
        out_specs=(P(("ex", "ft")), P(("ex", "ft"))),
        check_vma=False,
    )
```

```python
import functools
import itertools

import jax
import jax.numpy as jnp
from jax import lax
from jax.experimental import pallas as pl
from jax.experimental.pallas import tpu as pltpu
from jax.sharding import PartitionSpec as P

ITERS = 2
MESH = pl.DeviceIdType.MESH
HI = lax.Precision.HIGHEST
F32 = jnp.float32
BF16 = jnp.bfloat16
BATCHES = (8, 8, 8, 8, 8, 8, 8, 8)


def contract_last(a, b):
    return lax.dot_general(a, b, (((1,), (1,)), ((), ())), precision=HI, preferred_element_type=F32)


def hops(offset, sizes):
    return sum(min(o, n - o) for o, n in zip(offset, sizes))


def kernel(
    sizes, x_hbm, lab_hbm, w_hbm, s_hbm, y_hbm, out_ref,
    x_v, x_out, x_f, lab_ref, w_ref, s_v, y_v, w_own, wg, rs_send, rs_recv, ar_own, ar, gl, gtmp, gcore, gax,
    lab_send, lab_recv, m_send, m_recv, r_ref, t_ref, g_ref, gp_ref, d_ref,
    x_sem, xr_send, xr_recv, h_sem, ag_send, ag_recv, rs_sem, ar_sem, g_sem, l_sem, m_sem,
):
    ny, nx, nz = sizes
    plane = nx * nz
    chips = ny * plane
    m = s_v.shape[0]
    ex = lax.axis_index("ex")
    ft = lax.axis_index("ft")
    core = lax.rem(ft, 2)
    xz = ft // 2
    px, pz = xz // nz, lax.rem(xz, nz)
    chip = ex * plane + xz
    other = 1 - core
    partner = (ex, xz * 2 + other)

    steps = (plane, nz, 1)
    mine = (ex, px, pz)
    ahead = [[lax.rem(p + o, n) * d for o in range(n)] for p, n, d in zip(mine, sizes, steps)]
    behind = [[lax.rem(p + n - o, n) * d for o in range(n)] for p, n, d in zip(mine, sizes, steps)]

    def index(offset, table):
        return table[0][offset[0]] + table[1][offset[1]] + table[2][offset[2]]

    at_y = [lax.rem(ex + o, ny) for o in range(ny)]

    def peer(offset):
        return at_y[offset[0]], ahead[1][offset[1]] + ahead[2][offset[2]]

    def dest(place):
        return (place[0], place[1] * 2 + other)

    offsets = sorted(
        itertools.product(*map(range, sizes)),
        key=lambda o: -hops(o, sizes))
    rounds = chips // 8

    def round_of(offset):
        j = 0
        for o, n in zip(offset, sizes):
            j = 2 * j + (1 if n == 4 and o in (3, 0) else 0)
        return {3: 4, 4: 3}.get(j, j)

    def round_blocks(k, table):
        j = k + jnp.where(k == 3, 1, 0) - jnp.where(k == 4, 1, 0)
        lows = []
        for places, high in zip(table, (j // 4, lax.rem(j // 2, 2), lax.rem(j, 2))):
            if len(places) == 4:
                lows.append([jnp.where(high == 0, places[2], places[3]), jnp.where(high == 0, places[1], places[0])])
            else:
                lows.append([places[1], places[0]])
        return [a + b + c for a in lows[0] for b in lows[1] for c in lows[2]]

    def whole(ref, sem):
        return pltpu.make_async_copy(ref, ref, sem)

    hist = [
        pltpu.make_async_copy(s_hbm, s_v, h_sem.at[0]),
        pltpu.make_async_copy(y_hbm, y_v, h_sem.at[1]),
    ]
    small = [
        pltpu.make_async_copy(w_hbm, w_ref, h_sem.at[2]),
        pltpu.make_async_copy(lab_hbm, lab_ref, h_sem.at[3]),
    ]
    for copy in small + hist:
        copy.start()
    for h in range(2):
        pltpu.make_async_copy(x_hbm.at[h, :, core], x_out.at[:, h], x_sem.at[1]).start()
    for h in range(2):
        pltpu.make_async_copy(x_hbm.at[h, :, other], x_v.at[:, h], x_sem.at[0]).start()

    barrier = pltpu.get_barrier_semaphore()
    for offset in offsets:
        pl.semaphore_signal(barrier, inc=1, device_id=dest(peer(offset)), device_id_type=MESH)

    row8 = lax.broadcasted_iota(jnp.int32, (8, 128), 0)
    lanes8 = lax.broadcasted_iota(jnp.int32, (8, 128), 1)
    for copy in small:
        copy.wait()
    lab = jnp.zeros((8, 128), F32)
    for h in range(2):
        for e in range(8):
            value = lab_ref[h * 8 + e].astype(F32)
            lab = jnp.where((row8 == e), value, lab)
        lab_send[h] = lab
    w_own[0] = w_ref[...].astype(BF16)
    t_ref[...] = jnp.zeros_like(t_ref)
    gl[...] = jnp.zeros_like(gl)
    gtmp[...] = jnp.zeros_like(gtmp)
    for copy in hist:
        copy.wait()
    gl[0:m, 0:m] = contract_last(s_v[...], y_v[...])
    gtmp[0:m, 0:m] = contract_last(y_v[...], y_v[...])
    gcore[core] = gl[...] + pltpu.roll(gtmp[...], 64, 1)
    pl.semaphore_wait(barrier, chips)

    def gather_start(it):
        for offset in offsets:
            pltpu.make_async_remote_copy(
                src_ref=w_own.at[it], dst_ref=wg.at[it, chip],
                send_sem=ag_send.at[0], recv_sem=ag_recv.at[round_of(offset)],
                device_id=dest(peer(offset)), device_id_type=MESH).start()

    gather_start(0)

    def gram_send(stage):
        if stage == 3:
            pltpu.make_async_remote_copy(
                src_ref=gcore.at[core], dst_ref=gcore.at[core],
                send_sem=g_sem.at[4], recv_sem=g_sem.at[3],
                device_id=partner, device_id_type=MESH).start()
            return
        own = mine[stage]
        for off in range(1, sizes[stage]):
            offset = tuple(off if a == stage else 0 for a in range(3))
            pltpu.make_async_remote_copy(
                src_ref=gax.at[stage, own], dst_ref=gax.at[stage, own],
                send_sem=g_sem.at[5 + stage], recv_sem=g_sem.at[stage],
                device_id=dest(peer(offset)), device_id_type=MESH).start()

    def gram_sum(stage):
        if stage == 3:
            for i in (4, 3):
                whole(gcore.at[0], g_sem.at[i]).wait()
            return gcore[0] + gcore[1]
        for i in (5 + stage, stage):
            whole(gax.at[stage, pl.ds(0, sizes[stage] - 1)], g_sem.at[i]).wait()
        total = gax[stage, 0]
        for place in range(1, sizes[stage]):
            total = total + gax[stage, place]
        return total

    gram_send(3)
    whole(x_out, x_sem.at[1]).wait()
    for offset in reversed(offsets):
        c = index(offset, behind)
        pltpu.make_async_remote_copy(
            src_ref=x_out.at[c], dst_ref=x_v.at[c, 2:4],
            send_sem=xr_send.at[0], recv_sem=xr_recv.at[round_of(offset)],
            device_id=partner, device_id_type=MESH).start()
    lab_copy = pltpu.make_async_remote_copy(
        src_ref=lab_send, dst_ref=lab_recv, send_sem=l_sem.at[0], recv_sem=l_sem.at[1],
        device_id=partner, device_id_type=MESH)
    lab_copy.start()

    gax[0, ex] = gram_sum(3)
    gram_send(0)

    row16 = lax.broadcasted_iota(jnp.int32, (16, 128), 0)
    tile16 = lax.broadcasted_iota(jnp.int32, (16, 128), 1) // 8
    on_diag = row16 == tile16
    row24 = lax.broadcasted_iota(jnp.int32, (24, 128), 0)
    lane24 = lax.broadcasted_iota(jnp.int32, (24, 128), 1)
    row_m, lane_m = row24[0:m], lane24[0:m]
    lane1 = lax.broadcasted_iota(jnp.int32, (1, 128), 1)
    eye = jnp.where((row24 == lane24) & (row24 < m), 1.0, 0.0).astype(F32)
    turn = jnp.where(lax.rem(lanes8, 8) == row8, 1.0, 0.0).astype(F32)

    def margin_terms(it, blocks, accs):
        accs = list(accs)
        count = 3 if it == 0 else 4
        if it == 0:
            left = jnp.concatenate([wg[it, c] for c in blocks], axis=1)
            right = jnp.concatenate([x_v[c, 3] for c in blocks], axis=1)
            accs[6] = accs[6] + lax.dot_general(
                left, right, (((1,), (1,)), ((), ())), preferred_element_type=F32)
        for c in blocks:
            for t in range(0, 16, 2):
                w = wg[it, c, t:t + 2, :].astype(F32)
                w = jnp.concatenate(
                    [jnp.broadcast_to(w[0:1], (8, 128)), jnp.broadcast_to(w[1:2], (8, 128))], axis=0)
                for f in range(count):
                    if it == 0:
                        prod = x_v[c, f, t * 8:t * 8 + 16, :].astype(F32) * w
                    else:
                        prod = x_f[c, f, t * 8:t * 8 + 16, :] * w
                    accs[f] = accs[f] + prod[0:8]
                    accs[count + f] = accs[count + f] + prod[8:16]
        return tuple(accs)

    def zeros(count):
        return tuple(jnp.zeros((8, 128), F32) for _ in range(count))

    def lane_sums(accs):
        return [jnp.sum(acc, axis=1, keepdims=True) for acc in accs]

    weights = w_ref[...]
    rinv = rinvt = yy = diag = gamma0 = None
    for it in range(ITERS):
        if it == 0:
            whole(x_out, x_sem.at[0]).wait()

        groups, per = rounds, 1

        def arrive(i, accs):
            g = groups - 1 - i
            if it == 0:
                whole(x_out.at[pl.ds(0, 8 * per)], xr_recv.at[g]).wait()
            whole(wg.at[it, pl.ds(0, 8 * per)], ag_recv.at[g]).wait()
            return lax.fori_loop(
                0, per, lambda j, a: margin_terms(it, round_blocks(g * per + j, behind), a), accs)

        if it == 0:
            accs = arrive(0, zeros(6) + (jnp.zeros((16, 128), F32),))
            gax[1, px] = gram_sum(0)
            gram_send(1)
            accs = lax.fori_loop(1, groups, arrive, accs)
            line = jnp.sum(jnp.where(on_diag, accs[6], 0.0), axis=0, keepdims=True)
            cols = lane_sums([accs[f] + accs[3 + f] for f in range(3)] + [turn * line])
        else:
            accs = lax.fori_loop(0, groups, arrive, zeros(8))
            cols = lane_sums([accs[f] + accs[4 + f] for f in range(4)])
        for k in range(4):
            m_send[it, (k + 2) % 4] = jnp.broadcast_to(cols[k], (8, 128))
        m_copy = pltpu.make_async_remote_copy(
            src_ref=m_send.at[it], dst_ref=m_recv.at[it],
            send_sem=m_sem.at[0], recv_sem=m_sem.at[1],
            device_id=partner, device_id_type=MESH)
        m_copy.start()
        if it > 0:
            whole(ar.at[it - 1, pl.ds(0, 2 * chips - 1)], ar_sem.at[0]).wait()
        if it == 0:
            lab_copy.wait()
            lab_all = [lab_send[0], lab_send[1], lab_recv[0], lab_recv[1]]
        m_copy.wait()
        for k in range(4):
            resid = jax.nn.sigmoid(m_send[it, (k + 2) % 4] + m_recv[it, k]) - lab_all[k]
            line = jnp.sum(turn * resid, axis=0, keepdims=True)
            r_ref[:, k * 128:(k + 1) * 128] = jnp.where(on_diag, line, 0.0).astype(BF16)

        def scatter_send(batch):
            for offset in batch:
                pltpu.make_async_remote_copy(
                    src_ref=rs_send.at[it, index(offset, ahead)], dst_ref=rs_recv.at[it, chip],
                    send_sem=rs_sem.at[0], recv_sem=rs_sem.at[1],
                    device_id=dest(peer(offset)), device_id_type=MESH).start()

        lines = r_ref[...]
        start = 0
        for size in BATCHES[:1] if chips < 16 else BATCHES:
            batch = offsets[start:min(start + size, chips)]
            start += size
            for j in range(0, len(batch), 2):
                c0, c1 = index(batch[j], ahead), index(batch[j + 1], ahead)
                both = jnp.concatenate([x_v[c0].reshape(512, 128), x_v[c1].reshape(512, 128)], axis=1)
                term = jnp.dot(lines, both, preferred_element_type=F32).astype(BF16)
                rs_send[it, c0] = term[:, 0:128]
                rs_send[it, c1] = term[:, 128:256]
            scatter_send(batch)
            if it == 0 and start == (BATCHES[0] if chips < 16 else sum(BATCHES[:2])):
                gax[2, pz] = gram_sum(1)
                gram_send(2)
        if it == 0:
            total = gram_sum(2)
            upper = jnp.where((row24 <= lane24) & (lane24 < m), total, 0.0)
            yy = jnp.where((lane24 < m) & (row24 < m), pltpu.roll(total, 64, 1), 0.0)
            diag = upper * eye
            inv = eye
            for i in reversed(range(m)):
                line = inv[i:i + 1, :] / upper[i:i + 1, i:i + 1]
                column = jnp.where(row24[:, 0:1] < i, upper[:, i:i + 1], 0.0)
                inv = jnp.where(row24 == i, line, inv - column * line)
            rinv = inv
            t_ref[0:24, :] = inv
            rinvt = t_ref[...].T[0:24, :]
            gamma0 = upper[m - 1:m, m - 1:m] / yy[m - 1:m, m - 1:m]
        whole(wg.at[it], ag_send.at[0]).wait()
        whole(rs_recv.at[it], rs_sem.at[1]).wait()

        def add(k, total):
            return total + rs_recv[it, k].astype(F32)
        grad = lax.fori_loop(0, chips, add, jnp.zeros((16, 128), F32), unroll=8) + 0.1 * weights
        g_ref[...] = grad
        vectors = [g_ref]
        if it > 0:
            gp_ref[...] = grad - gp_ref[...]
            vectors.append(gp_ref)
            for t in range(16):
                y_v[0:1, t * 128:(t + 1) * 128] = gp_ref[t:t + 1, :]
        sums = jnp.zeros((m, 128), F32)
        for v, vec in enumerate(vectors):
            acc_s = jnp.zeros((m, 128), F32)
            acc_y = jnp.zeros((m, 128), F32)
            for t in range(16):
                line = vec[t:t + 1, :]
                acc_s = acc_s + s_v[:, t * 128:(t + 1) * 128] * line
                acc_y = acc_y + y_v[:, t * 128:(t + 1) * 128] * line
            for part, acc in ((2 * v, acc_s), (2 * v + 1, acc_y)):
                own_lane = lane_m == row_m + 32 * part
                sums = sums + jnp.where(own_lane, jnp.sum(acc, axis=1, keepdims=True), 0.0)
        sums = jnp.sum(sums, axis=0, keepdims=True)
        ar_own[it] = sums
        ar[it, chip * 2 + core] = sums

        def total_send(device):
            pltpu.make_async_remote_copy(
                src_ref=ar_own.at[it], dst_ref=ar.at[it, chip * 2 + core],
                send_sem=ar_sem.at[0], recv_sem=ar_sem.at[1],
                device_id=device, device_id_type=MESH).start()

        for offset in offsets[:-1]:
            cy, cxz = peer(offset)
            total_send((cy, cxz * 2))
            total_send((cy, cxz * 2 + 1))
        total_send(partner)
        if it == 0:
            def widen(c, carry):
                x_f[c] = x_v[c].astype(F32)
                return carry
            lax.fori_loop(0, chips, widen, 0)
        whole(rs_send.at[it], rs_sem.at[0]).wait()
        whole(ar.at[it, pl.ds(0, 2 * chips - 1)], ar_sem.at[1]).wait()
        tot = jnp.broadcast_to(jnp.sum(ar[it], axis=0), (8, 128))
        u, hh = tot[0:1], pltpu.roll(tot, 96, 1)[0:1]
        if it == 0:
            gamma = gamma0
            alpha = -jnp.sum(rinv * u, axis=1, keepdims=True)
            p = gamma * (jnp.sum(yy * alpha, axis=0, keepdims=True) + hh)
            p = p + jnp.sum(diag * alpha, axis=0, keepdims=True)
            coef = jnp.sum(rinvt * p, axis=1, keepdims=True)
        else:
            v, z = pltpu.roll(tot, 64, 1)[0:1], pltpu.roll(tot, 32, 1)[0:1]
            v0, z0, u0 = v[:, 0:1], z[:, 0:1], u[:, 0:1]
            gamma = v0 / z0
            a0 = -u0 / v0
            old = (row24 > 0) & (lane24 > 0)
            rm, rmt = jnp.where(old, rinv, 0.0), jnp.where(old, rinvt, 0.0)
            ru = jnp.sum(rm * u, axis=1, keepdims=True)
            rv = jnp.sum(rm * v, axis=1, keepdims=True)
            rv_flat = jnp.sum(eye * rv, axis=0, keepdims=True)
            alpha = jnp.where(row24[:, 0:1] == 0, a0, -(ru + rv * a0))
            flat = jnp.sum(eye * alpha, axis=0, keepdims=True)
            newest = jnp.sum(jnp.where(lane1 < m, z, 0.0) * flat, axis=1, keepdims=True)
            q = jnp.sum(jnp.where(old, yy, 0.0) * alpha, axis=0, keepdims=True) + z * a0
            p = gamma * (q + hh) + jnp.sum(diag * alpha, axis=0, keepdims=True)
            coef = jnp.sum(rmt * p, axis=1, keepdims=True)
            rest = jnp.sum(rv_flat * p, axis=1, keepdims=True)
            c0 = (gamma * (newest + hh[:, 0:1]) + v0 * a0 - rest) / v0
            coef = jnp.where(row24[:, 0:1] == 0, c0, coef)
        cs, cy = coef[0:m], (-gamma * alpha)[0:m]
        for t in range(16):
            cols = slice(t * 128, (t + 1) * 128)
            d_ref[t:t + 1, :] = jnp.sum(cs * s_v[:, cols] + cy * y_v[:, cols], axis=0, keepdims=True)
        direction = d_ref[...] - gamma * g_ref[...]
        new = weights + direction
        if it < ITERS - 1:
            w_own[it + 1] = new.astype(BF16)
            gather_start(it + 1)
            gp_ref[...] = grad
            d_ref[...] = new - weights
            for t in range(16):
                s_v[0:1, t * 128:(t + 1) * 128] = d_ref[t:t + 1, :]
            weights = new
        else:
            out_ref[0] = new
            out_ref[1] = direction

    whole(x_out, xr_send.at[0]).wait()
    whole(ar.at[0, pl.ds(0, 2 * chips - 1)], ar_sem.at[0]).wait()


def per_device(sizes, features, labels, start_weights, hist_s, hist_y):
    ny, nx, nz = sizes
    chips = ny * nx * nz
    m = hist_s.shape[0]
    x = features.reshape(2, 8, chips, 2, 16, 128).transpose(0, 2, 3, 4, 1, 5)
    x = x.reshape(2, chips, 2, 128, 128)
    vmem = pl.BlockSpec(memory_space=pltpu.VMEM)
    hbm = pl.BlockSpec(memory_space=pl.ANY)
    dma = pltpu.SemaphoreType.DMA
    out = pl.pallas_call(
        functools.partial(kernel, sizes),
        out_shape=pltpu.VMEM((2, 16, 128), F32),
        in_specs=[hbm] * 5,
        out_specs=vmem,
        scratch_shapes=[
            pltpu.VMEM((chips, 4, 128, 128), BF16),
            pltpu.VMEM((chips, 2, 128, 128), BF16),
            pltpu.VMEM((chips, 4, 128, 128), F32),
            pltpu.SMEM((16,), jnp.int32),
            pltpu.VMEM((16, 128), F32),
            pltpu.VMEM((m, 2048), F32),
            pltpu.VMEM((m, 2048), F32),
            pltpu.VMEM((ITERS, 16, 128), BF16),
            pltpu.VMEM((ITERS, chips, 16, 128), BF16),
            pltpu.VMEM((ITERS, chips, 16, 128), BF16),
            pltpu.VMEM((ITERS, chips, 16, 128), BF16),
            pltpu.VMEM((ITERS, 1, 128), F32),
            pltpu.VMEM((ITERS, 2 * chips, 1, 128), F32),
            pltpu.VMEM((24, 128), F32),
            pltpu.VMEM((24, 128), F32),
            pltpu.VMEM((2, 24, 128), F32),
            pltpu.VMEM((3, 4, 24, 128), F32),
            pltpu.VMEM((2, 8, 128), F32),
            pltpu.VMEM((2, 8, 128), F32),
            pltpu.VMEM((ITERS, 4, 8, 128), F32),
            pltpu.VMEM((ITERS, 4, 8, 128), F32),
            pltpu.VMEM((16, 512), BF16),
            pltpu.VMEM((128, 128), F32),
            pltpu.VMEM((16, 128), F32),
            pltpu.VMEM((16, 128), F32),
            pltpu.VMEM((16, 128), F32),
            dma((2,)), dma((1,)), dma((chips // 8,)), dma((4,)), dma((1,)), dma((chips // 8,)),
            dma((2,)), dma((2,)), dma((8,)), dma((2,)), dma((2,)),
        ],
        compiler_params=pltpu.CompilerParams(collective_id=0, has_side_effects=True),
    )(x, labels, start_weights.reshape(16, 128), hist_s, hist_y)
    out = out.reshape(2, 2048)
    return out[0], out[1]


def solution(mesh):
    ny, rest = mesh.shape["ex"], mesh.shape["ft"] // 2
    nx = round(rest ** 0.5)
    sizes = (ny, nx, rest // nx)
    return jax.shard_map(
        functools.partial(per_device, sizes),
        mesh=mesh,
        in_specs=(
            P(("ex", "ft"), None),
            P(("ex", "ft")),
            P(("ex", "ft")),
            P(None, ("ex", "ft")),
            P(None, ("ex", "ft")),
        ),
        out_specs=(P(("ex", "ft")), P(("ex", "ft"))),
        check_vma=False,
    )
```

```python
import functools
import itertools

import jax
import jax.numpy as jnp
from jax import lax
from jax.experimental import pallas as pl
from jax.experimental.pallas import tpu as pltpu
from jax.sharding import PartitionSpec as P

ITERS = 2
MESH = pl.DeviceIdType.MESH
HI = lax.Precision.HIGHEST
F32 = jnp.float32
BF16 = jnp.bfloat16
BATCHES = (8, 8, 8, 8, 8, 8, 8, 8)


def contract_last(a, b):
    return lax.dot_general(a, b, (((1,), (1,)), ((), ())), precision=HI, preferred_element_type=F32)


def hops(offset, sizes):
    return sum(min(o, n - o) for o, n in zip(offset, sizes))


def kernel(
    sizes, x_hbm, lab_hbm, w_hbm, s_hbm, y_hbm, out_ref,
    x_v, x_out, x_f, lab_ref, w_ref, s_v, y_v, w_own, wg, rs_send, rs_recv, ar_own, ar, gl, gtmp, gcore, gax,
    lab_send, lab_recv, m_send, m_recv, r_ref, t_ref, g_ref, gp_ref, d_ref, rs_f, data_ref,
    x_sem, xr_send, xr_recv, h_sem, ag_send, ag_recv, rs_sem, ar_sem, g_sem, l_sem, m_sem,
):
    ny, nx, nz = sizes
    plane = nx * nz
    chips = ny * plane
    m = s_v.shape[0]
    ex = lax.axis_index("ex")
    ft = lax.axis_index("ft")
    core = lax.rem(ft, 2)
    xz = ft // 2
    px, pz = xz // nz, lax.rem(xz, nz)
    chip = ex * plane + xz
    other = 1 - core
    partner = (ex, xz * 2 + other)

    steps = (plane, nz, 1)
    mine = (ex, px, pz)
    ahead = [[lax.rem(p + o, n) * d for o in range(n)] for p, n, d in zip(mine, sizes, steps)]
    behind = [[lax.rem(p + n - o, n) * d for o in range(n)] for p, n, d in zip(mine, sizes, steps)]

    def index(offset, table):
        return table[0][offset[0]] + table[1][offset[1]] + table[2][offset[2]]

    at_y = [lax.rem(ex + o, ny) for o in range(ny)]

    def peer(offset):
        return at_y[offset[0]], ahead[1][offset[1]] + ahead[2][offset[2]]

    def dest(place):
        return (place[0], place[1] * 2 + other)

    offsets = sorted(
        itertools.product(*map(range, sizes)),
        key=lambda o: -hops(o, sizes))
    rounds = chips // 8

    def round_of(offset):
        j = 0
        for o, n in zip(offset, sizes):
            j = 2 * j + (1 if n == 4 and o in (3, 0) else 0)
        return {3: 4, 4: 3}.get(j, j)

    def round_blocks(k, table):
        j = k + jnp.where(k == 3, 1, 0) - jnp.where(k == 4, 1, 0)
        lows = []
        for places, high in zip(table, (j // 4, lax.rem(j // 2, 2), lax.rem(j, 2))):
            if len(places) == 4:
                lows.append([jnp.where(high == 0, places[2], places[3]), jnp.where(high == 0, places[1], places[0])])
            else:
                lows.append([places[1], places[0]])
        return [a + b + c for a in lows[0] for b in lows[1] for c in lows[2]]

    def whole(ref, sem):
        return pltpu.make_async_copy(ref, ref, sem)

    hist = [
        pltpu.make_async_copy(s_hbm, s_v, h_sem.at[0]),
        pltpu.make_async_copy(y_hbm, y_v, h_sem.at[1]),
    ]
    small = [
        pltpu.make_async_copy(w_hbm, w_ref, h_sem.at[2]),
        pltpu.make_async_copy(lab_hbm, lab_ref, h_sem.at[3]),
    ]
    for copy in small + hist:
        copy.start()
    for h in range(2):
        pltpu.make_async_copy(x_hbm.at[h, :, core], x_out.at[:, h], x_sem.at[1]).start()
    for h in range(2):
        pltpu.make_async_copy(x_hbm.at[h, :, other], x_v.at[:, h], x_sem.at[0]).start()

    barrier = pltpu.get_barrier_semaphore()
    for offset in offsets:
        pl.semaphore_signal(barrier, inc=1, device_id=dest(peer(offset)), device_id_type=MESH)

    row8 = lax.broadcasted_iota(jnp.int32, (8, 128), 0)
    lanes8 = lax.broadcasted_iota(jnp.int32, (8, 128), 1)
    for copy in small:
        copy.wait()
    lab = jnp.zeros((8, 128), F32)
    for h in range(2):
        for e in range(8):
            value = lab_ref[h * 8 + e].astype(F32)
            lab = jnp.where((row8 == e), value, lab)
        lab_send[h] = lab
    w_own[0] = w_ref[...].astype(BF16)
    t_ref[...] = jnp.zeros_like(t_ref)
    gl[...] = jnp.zeros_like(gl)
    gtmp[...] = jnp.zeros_like(gtmp)
    for copy in hist:
        copy.wait()
    gl[0:m, 0:m] = contract_last(s_v[...], y_v[...])
    gtmp[0:m, 0:m] = contract_last(y_v[...], y_v[...])
    gcore[core] = gl[...] + pltpu.roll(gtmp[...], 64, 1)
    pl.semaphore_wait(barrier, chips)

    def gather_start(it):
        for offset in offsets:
            pltpu.make_async_remote_copy(
                src_ref=w_own.at[it], dst_ref=wg.at[it, chip],
                send_sem=ag_send.at[0], recv_sem=ag_recv.at[round_of(offset)],
                device_id=dest(peer(offset)), device_id_type=MESH).start()

    gather_start(0)

    def gram_send(stage):
        if stage == 3:
            pltpu.make_async_remote_copy(
                src_ref=gcore.at[core], dst_ref=gcore.at[core],
                send_sem=g_sem.at[4], recv_sem=g_sem.at[3],
                device_id=partner, device_id_type=MESH).start()
            return
        own = mine[stage]
        for off in range(1, sizes[stage]):
            offset = tuple(off if a == stage else 0 for a in range(3))
            pltpu.make_async_remote_copy(
                src_ref=gax.at[stage, own], dst_ref=gax.at[stage, own],
                send_sem=g_sem.at[5 + stage], recv_sem=g_sem.at[stage],
                device_id=dest(peer(offset)), device_id_type=MESH).start()

    def gram_sum(stage):
        if stage == 3:
            for i in (4, 3):
                whole(gcore.at[0], g_sem.at[i]).wait()
            return gcore[0] + gcore[1]
        for i in (5 + stage, stage):
            whole(gax.at[stage, pl.ds(0, sizes[stage] - 1)], g_sem.at[i]).wait()
        total = gax[stage, 0]
        for place in range(1, sizes[stage]):
            total = total + gax[stage, place]
        return total

    gram_send(3)
    whole(x_out, x_sem.at[1]).wait()
    for offset in reversed(offsets):
        c = index(offset, behind)
        pltpu.make_async_remote_copy(
            src_ref=x_out.at[c], dst_ref=x_v.at[c, 2:4],
            send_sem=xr_send.at[0], recv_sem=xr_recv.at[round_of(offset)],
            device_id=partner, device_id_type=MESH).start()
    lab_copy = pltpu.make_async_remote_copy(
        src_ref=lab_send, dst_ref=lab_recv, send_sem=l_sem.at[0], recv_sem=l_sem.at[1],
        device_id=partner, device_id_type=MESH)
    lab_copy.start()

    gax[0, ex] = gram_sum(3)
    gram_send(0)

    row16 = lax.broadcasted_iota(jnp.int32, (16, 128), 0)
    tile16 = lax.broadcasted_iota(jnp.int32, (16, 128), 1) // 8
    on_diag = row16 == tile16
    row24 = lax.broadcasted_iota(jnp.int32, (24, 128), 0)
    lane24 = lax.broadcasted_iota(jnp.int32, (24, 128), 1)
    row_m, lane_m = row24[0:m], lane24[0:m]
    lane1 = lax.broadcasted_iota(jnp.int32, (1, 128), 1)
    eye = jnp.where((row24 == lane24) & (row24 < m), 1.0, 0.0).astype(F32)
    turn = jnp.where(lax.rem(lanes8, 8) == row8, 1.0, 0.0).astype(F32)

    def margin_terms(it, blocks, accs):
        accs = list(accs)
        count = 3 if it == 0 else 4
        if it == 0:
            left = jnp.concatenate([wg[it, c] for c in blocks], axis=1)
            right = jnp.concatenate([x_v[c, 3] for c in blocks], axis=1)
            accs[6] = accs[6] + lax.dot_general(
                left, right, (((1,), (1,)), ((), ())), preferred_element_type=F32)
        for c in blocks:
            for t in range(0, 16, 2):
                w = wg[it, c, t:t + 2, :].astype(F32)
                w = jnp.concatenate(
                    [jnp.broadcast_to(w[0:1], (8, 128)), jnp.broadcast_to(w[1:2], (8, 128))], axis=0)
                for f in range(count):
                    if it == 0:
                        prod = x_v[c, f, t * 8:t * 8 + 16, :].astype(F32) * w
                    else:
                        prod = x_f[c, f, t * 8:t * 8 + 16, :] * w
                    accs[f] = accs[f] + prod[0:8]
                    accs[count + f] = accs[count + f] + prod[8:16]
        return tuple(accs)

    def zeros(count):
        return tuple(jnp.zeros((8, 128), F32) for _ in range(count))

    def lane_sums(accs):
        return [jnp.sum(acc, axis=1, keepdims=True) for acc in accs]

    weights = w_ref[...]
    rinv = rinvt = yy = diag = gamma0 = None
    for it in range(ITERS):
        if it == 0:
            whole(x_out, x_sem.at[0]).wait()

        groups, per = rounds, 1

        def arrive(i, accs):
            g = groups - 1 - i
            if it == 0:
                whole(x_out.at[pl.ds(0, 8 * per)], xr_recv.at[g]).wait()
            whole(wg.at[it, pl.ds(0, 8 * per)], ag_recv.at[g]).wait()
            return lax.fori_loop(
                0, per, lambda j, a: margin_terms(it, round_blocks(g * per + j, behind), a), accs)

        if it == 0:
            accs = arrive(0, zeros(6) + (jnp.zeros((16, 128), F32),))
            gax[1, px] = gram_sum(0)
            gram_send(1)
            accs = lax.fori_loop(1, groups, arrive, accs)
            line = jnp.sum(jnp.where(on_diag, accs[6], 0.0), axis=0, keepdims=True)
            cols = lane_sums([accs[f] + accs[3 + f] for f in range(3)] + [turn * line])
        else:
            accs = lax.fori_loop(0, groups, arrive, zeros(8))
            cols = lane_sums([accs[f] + accs[4 + f] for f in range(4)])
        for k in range(4):
            m_send[it, (k + 2) % 4] = jnp.broadcast_to(cols[k], (8, 128))
        m_copy = pltpu.make_async_remote_copy(
            src_ref=m_send.at[it], dst_ref=m_recv.at[it],
            send_sem=m_sem.at[0], recv_sem=m_sem.at[1],
            device_id=partner, device_id_type=MESH)
        m_copy.start()
        if it > 0:
            whole(ar.at[it - 1, pl.ds(0, 2 * chips - 1)], ar_sem.at[0]).wait()
        if it == 0:
            lab_copy.wait()
            lab_all = [lab_send[0], lab_send[1], lab_recv[0], lab_recv[1]]
        m_copy.wait()
        for k in range(4):
            resid = jax.nn.sigmoid(m_send[it, (k + 2) % 4] + m_recv[it, k]) - lab_all[k]
            line = jnp.sum(turn * resid, axis=0, keepdims=True)
            r_ref[:, k * 128:(k + 1) * 128] = jnp.where(on_diag, line, 0.0).astype(BF16)

        def scatter_send(batch):
            for offset in batch:
                pltpu.make_async_remote_copy(
                    src_ref=rs_send.at[it, index(offset, ahead)], dst_ref=rs_recv.at[it, chip],
                    send_sem=rs_sem.at[0], recv_sem=rs_sem.at[1],
                    device_id=dest(peer(offset)), device_id_type=MESH).start()

        lines = r_ref[...]
        start = 0
        for size in BATCHES[:1] if chips < 16 else BATCHES:
            batch = offsets[start:min(start + size, chips)]
            start += size
            for j in range(0, len(batch), 2):
                c0, c1 = index(batch[j], ahead), index(batch[j + 1], ahead)
                both = jnp.concatenate([x_v[c0].reshape(512, 128), x_v[c1].reshape(512, 128)], axis=1)
                term = jnp.dot(lines, both, preferred_element_type=F32)
                for c, part in ((c0, term[:, 0:128]), (c1, term[:, 128:256])):
                    if it == 0:
                        rs_f[c] = part
                    else:
                        part = part - rs_f[c]
                    rs_send[it, c] = part.astype(BF16)
            scatter_send(batch)
            if it == 0 and start == (BATCHES[0] if chips < 16 else sum(BATCHES[:2])):
                gax[2, pz] = gram_sum(1)
                gram_send(2)
        if it == 0:
            total = gram_sum(2)
            upper = jnp.where((row24 <= lane24) & (lane24 < m), total, 0.0)
            yy = jnp.where((lane24 < m) & (row24 < m), pltpu.roll(total, 64, 1), 0.0)
            diag = upper * eye
            inv = eye
            for i in reversed(range(m)):
                line = inv[i:i + 1, :] / upper[i:i + 1, i:i + 1]
                column = jnp.where(row24[:, 0:1] < i, upper[:, i:i + 1], 0.0)
                inv = jnp.where(row24 == i, line, inv - column * line)
            rinv = inv
            t_ref[0:24, :] = inv
            rinvt = t_ref[...].T[0:24, :]
            gamma0 = upper[m - 1:m, m - 1:m] / yy[m - 1:m, m - 1:m]
        whole(wg.at[it], ag_send.at[0]).wait()
        whole(rs_recv.at[it], rs_sem.at[1]).wait()

        def add(k, total):
            return total + rs_recv[it, k].astype(F32)
        total = lax.fori_loop(0, chips, add, jnp.zeros((16, 128), F32) if it == 0 else data_ref[...], unroll=8)
        if it == 0:
            data_ref[...] = total
        grad = total + 0.1 * weights
        g_ref[...] = grad
        vectors = [g_ref]
        if it > 0:
            gp_ref[...] = grad - gp_ref[...]
            vectors.append(gp_ref)
            for t in range(16):
                y_v[0:1, t * 128:(t + 1) * 128] = gp_ref[t:t + 1, :]
        sums = jnp.zeros((m, 128), F32)
        for v, vec in enumerate(vectors):
            acc_s = jnp.zeros((m, 128), F32)
            acc_y = jnp.zeros((m, 128), F32)
            for t in range(16):
                line = vec[t:t + 1, :]
                acc_s = acc_s + s_v[:, t * 128:(t + 1) * 128] * line
                acc_y = acc_y + y_v[:, t * 128:(t + 1) * 128] * line
            for part, acc in ((2 * v, acc_s), (2 * v + 1, acc_y)):
                own_lane = lane_m == row_m + 32 * part
                sums = sums + jnp.where(own_lane, jnp.sum(acc, axis=1, keepdims=True), 0.0)
        sums = jnp.sum(sums, axis=0, keepdims=True)
        ar_own[it] = sums
        ar[it, chip * 2 + core] = sums

        def total_send(device):
            pltpu.make_async_remote_copy(
                src_ref=ar_own.at[it], dst_ref=ar.at[it, chip * 2 + core],
                send_sem=ar_sem.at[0], recv_sem=ar_sem.at[1],
                device_id=device, device_id_type=MESH).start()

        for offset in offsets[:-1]:
            cy, cxz = peer(offset)
            total_send((cy, cxz * 2))
            total_send((cy, cxz * 2 + 1))
        total_send(partner)
        if it == 0:
            def widen(c, carry):
                x_f[c] = x_v[c].astype(F32)
                return carry
            lax.fori_loop(0, chips, widen, 0)
        whole(rs_send.at[it], rs_sem.at[0]).wait()
        whole(ar.at[it, pl.ds(0, 2 * chips - 1)], ar_sem.at[1]).wait()
        tot = jnp.broadcast_to(jnp.sum(ar[it], axis=0), (8, 128))
        u, hh = tot[0:1], pltpu.roll(tot, 96, 1)[0:1]
        if it == 0:
            gamma = gamma0
            alpha = -jnp.sum(rinv * u, axis=1, keepdims=True)
            p = gamma * (jnp.sum(yy * alpha, axis=0, keepdims=True) + hh)
            p = p + jnp.sum(diag * alpha, axis=0, keepdims=True)
            coef = jnp.sum(rinvt * p, axis=1, keepdims=True)
        else:
            v, z = pltpu.roll(tot, 64, 1)[0:1], pltpu.roll(tot, 32, 1)[0:1]
            v0, z0, u0 = v[:, 0:1], z[:, 0:1], u[:, 0:1]
            gamma = v0 / z0
            a0 = -u0 / v0
            old = (row24 > 0) & (lane24 > 0)
            rm, rmt = jnp.where(old, rinv, 0.0), jnp.where(old, rinvt, 0.0)
            ru = jnp.sum(rm * u, axis=1, keepdims=True)
            rv = jnp.sum(rm * v, axis=1, keepdims=True)
            rv_flat = jnp.sum(eye * rv, axis=0, keepdims=True)
            alpha = jnp.where(row24[:, 0:1] == 0, a0, -(ru + rv * a0))
            flat = jnp.sum(eye * alpha, axis=0, keepdims=True)
            newest = jnp.sum(jnp.where(lane1 < m, z, 0.0) * flat, axis=1, keepdims=True)
            q = jnp.sum(jnp.where(old, yy, 0.0) * alpha, axis=0, keepdims=True) + z * a0
            p = gamma * (q + hh) + jnp.sum(diag * alpha, axis=0, keepdims=True)
            coef = jnp.sum(rmt * p, axis=1, keepdims=True)
            rest = jnp.sum(rv_flat * p, axis=1, keepdims=True)
            c0 = (gamma * (newest + hh[:, 0:1]) + v0 * a0 - rest) / v0
            coef = jnp.where(row24[:, 0:1] == 0, c0, coef)
        cs, cy = coef[0:m], (-gamma * alpha)[0:m]
        for t in range(16):
            cols = slice(t * 128, (t + 1) * 128)
            d_ref[t:t + 1, :] = jnp.sum(cs * s_v[:, cols] + cy * y_v[:, cols], axis=0, keepdims=True)
        direction = d_ref[...] - gamma * g_ref[...]
        new = weights + direction
        if it < ITERS - 1:
            w_own[it + 1] = new.astype(BF16)
            gather_start(it + 1)
            gp_ref[...] = grad
            d_ref[...] = new - weights
            for t in range(16):
                s_v[0:1, t * 128:(t + 1) * 128] = d_ref[t:t + 1, :]
            weights = new
        else:
            out_ref[0] = new
            out_ref[1] = direction

    whole(x_out, xr_send.at[0]).wait()
    whole(ar.at[0, pl.ds(0, 2 * chips - 1)], ar_sem.at[0]).wait()


def per_device(sizes, features, labels, start_weights, hist_s, hist_y):
    ny, nx, nz = sizes
    chips = ny * nx * nz
    m = hist_s.shape[0]
    x = features.reshape(2, 8, chips, 2, 16, 128).transpose(0, 2, 3, 4, 1, 5)
    x = x.reshape(2, chips, 2, 128, 128)
    vmem = pl.BlockSpec(memory_space=pltpu.VMEM)
    hbm = pl.BlockSpec(memory_space=pl.ANY)
    dma = pltpu.SemaphoreType.DMA
    out = pl.pallas_call(
        functools.partial(kernel, sizes),
        out_shape=pltpu.VMEM((2, 16, 128), F32),
        in_specs=[hbm] * 5,
        out_specs=vmem,
        scratch_shapes=[
            pltpu.VMEM((chips, 4, 128, 128), BF16),
            pltpu.VMEM((chips, 2, 128, 128), BF16),
            pltpu.VMEM((chips, 4, 128, 128), F32),
            pltpu.SMEM((16,), jnp.int32),
            pltpu.VMEM((16, 128), F32),
            pltpu.VMEM((m, 2048), F32),
            pltpu.VMEM((m, 2048), F32),
            pltpu.VMEM((ITERS, 16, 128), BF16),
            pltpu.VMEM((ITERS, chips, 16, 128), BF16),
            pltpu.VMEM((ITERS, chips, 16, 128), BF16),
            pltpu.VMEM((ITERS, chips, 16, 128), BF16),
            pltpu.VMEM((ITERS, 1, 128), F32),
            pltpu.VMEM((ITERS, 2 * chips, 1, 128), F32),
            pltpu.VMEM((24, 128), F32),
            pltpu.VMEM((24, 128), F32),
            pltpu.VMEM((2, 24, 128), F32),
            pltpu.VMEM((3, 4, 24, 128), F32),
            pltpu.VMEM((2, 8, 128), F32),
            pltpu.VMEM((2, 8, 128), F32),
            pltpu.VMEM((ITERS, 4, 8, 128), F32),
            pltpu.VMEM((ITERS, 4, 8, 128), F32),
            pltpu.VMEM((16, 512), BF16),
            pltpu.VMEM((128, 128), F32),
            pltpu.VMEM((16, 128), F32),
            pltpu.VMEM((16, 128), F32),
            pltpu.VMEM((16, 128), F32),
            pltpu.VMEM((chips, 16, 128), F32),
            pltpu.VMEM((16, 128), F32),
            dma((2,)), dma((1,)), dma((chips // 8,)), dma((4,)), dma((1,)), dma((chips // 8,)),
            dma((2,)), dma((2,)), dma((8,)), dma((2,)), dma((2,)),
        ],
        compiler_params=pltpu.CompilerParams(collective_id=0, has_side_effects=True),
    )(x, labels, start_weights.reshape(16, 128), hist_s, hist_y)
    out = out.reshape(2, 2048)
    return out[0], out[1]


def solution(mesh):
    ny, rest = mesh.shape["ex"], mesh.shape["ft"] // 2
    nx = round(rest ** 0.5)
    sizes = (ny, nx, rest // nx)
    return jax.shard_map(
        functools.partial(per_device, sizes),
        mesh=mesh,
        in_specs=(
            P(("ex", "ft"), None),
            P(("ex", "ft")),
            P(("ex", "ft")),
            P(None, ("ex", "ft")),
            P(None, ("ex", "ft")),
        ),
        out_specs=(P(("ex", "ft")), P(("ex", "ft"))),
        check_vma=False,
    )
```

```python
import functools
import itertools

import jax
import jax.numpy as jnp
from jax import lax
from jax.experimental import pallas as pl
from jax.experimental.pallas import tpu as pltpu
from jax.sharding import PartitionSpec as P

ITERS = 2
MESH = pl.DeviceIdType.MESH
HI = lax.Precision.HIGHEST
F32 = jnp.float32
BF16 = jnp.bfloat16
BATCHES = (8, 8, 8, 8, 8, 8, 8, 8)


def contract_last(a, b):
    return lax.dot_general(a, b, (((1,), (1,)), ((), ())), precision=HI, preferred_element_type=F32)


def hops(offset, sizes):
    return sum(min(o, n - o) for o, n in zip(offset, sizes))


def kernel(
    sizes, x_hbm, lab_hbm, w_hbm, s_hbm, y_hbm, out_ref,
    x_v, x_out, x_f, lab_ref, w_ref, s_v, y_v, w_own, wg, rs_send, rs_recv, ar_own, ar, gl, gtmp, gcore, gax,
    lab_send, lab_recv, m_send, m_recv, r_ref, t_ref, g_ref, gp_ref, d_ref, data_ref,
    x_sem, xr_send, xr_recv, h_sem, ag_send, ag_recv, rs_sem, ar_sem, g_sem, l_sem, m_sem,
):
    ny, nx, nz = sizes
    plane = nx * nz
    chips = ny * plane
    m = s_v.shape[0]
    ex = lax.axis_index("ex")
    ft = lax.axis_index("ft")
    core = lax.rem(ft, 2)
    xz = ft // 2
    px, pz = xz // nz, lax.rem(xz, nz)
    chip = ex * plane + xz
    other = 1 - core
    partner = (ex, xz * 2 + other)

    steps = (plane, nz, 1)
    mine = (ex, px, pz)
    ahead = [[lax.rem(p + o, n) * d for o in range(n)] for p, n, d in zip(mine, sizes, steps)]
    behind = [[lax.rem(p + n - o, n) * d for o in range(n)] for p, n, d in zip(mine, sizes, steps)]

    def index(offset, table):
        return table[0][offset[0]] + table[1][offset[1]] + table[2][offset[2]]

    at_y = [lax.rem(ex + o, ny) for o in range(ny)]

    def peer(offset):
        return at_y[offset[0]], ahead[1][offset[1]] + ahead[2][offset[2]]

    def dest(place):
        return (place[0], place[1] * 2 + other)

    offsets = sorted(
        itertools.product(*map(range, sizes)),
        key=lambda o: -hops(o, sizes))
    rounds = chips // 8

    def round_of(offset):
        j = 0
        for o, n in zip(offset, sizes):
            j = 2 * j + (1 if n == 4 and o in (3, 0) else 0)
        return {3: 4, 4: 3}.get(j, j)

    def round_blocks(k, table):
        j = k + jnp.where(k == 3, 1, 0) - jnp.where(k == 4, 1, 0)
        lows = []
        for places, high in zip(table, (j // 4, lax.rem(j // 2, 2), lax.rem(j, 2))):
            if len(places) == 4:
                lows.append([jnp.where(high == 0, places[2], places[3]), jnp.where(high == 0, places[1], places[0])])
            else:
                lows.append([places[1], places[0]])
        return [a + b + c for a in lows[0] for b in lows[1] for c in lows[2]]

    def whole(ref, sem):
        return pltpu.make_async_copy(ref, ref, sem)

    hist = [
        pltpu.make_async_copy(s_hbm, s_v, h_sem.at[0]),
        pltpu.make_async_copy(y_hbm, y_v, h_sem.at[1]),
    ]
    small = [
        pltpu.make_async_copy(w_hbm, w_ref, h_sem.at[2]),
        pltpu.make_async_copy(lab_hbm, lab_ref, h_sem.at[3]),
    ]
    for copy in small + hist:
        copy.start()
    for h in range(2):
        pltpu.make_async_copy(x_hbm.at[h, :, core], x_out.at[:, h], x_sem.at[1]).start()
    for h in range(2):
        pltpu.make_async_copy(x_hbm.at[h, :, other], x_v.at[:, h], x_sem.at[0]).start()

    barrier = pltpu.get_barrier_semaphore()
    for offset in offsets:
        pl.semaphore_signal(barrier, inc=1, device_id=dest(peer(offset)), device_id_type=MESH)

    row8 = lax.broadcasted_iota(jnp.int32, (8, 128), 0)
    lanes8 = lax.broadcasted_iota(jnp.int32, (8, 128), 1)
    for copy in small:
        copy.wait()
    lab = jnp.zeros((8, 128), F32)
    for h in range(2):
        for e in range(8):
            value = lab_ref[h * 8 + e].astype(F32)
            lab = jnp.where((row8 == e), value, lab)
        lab_send[h] = lab
    w_own[0] = w_ref[...].astype(BF16)
    t_ref[...] = jnp.zeros_like(t_ref)
    gl[...] = jnp.zeros_like(gl)
    gtmp[...] = jnp.zeros_like(gtmp)
    for copy in hist:
        copy.wait()
    gl[0:m, 0:m] = contract_last(s_v[...], y_v[...])
    gtmp[0:m, 0:m] = contract_last(y_v[...], y_v[...])
    gcore[core] = gl[...] + pltpu.roll(gtmp[...], 64, 1)
    pl.semaphore_wait(barrier, chips)

    def gather_start(it):
        for offset in offsets:
            pltpu.make_async_remote_copy(
                src_ref=w_own.at[it], dst_ref=wg.at[it, chip],
                send_sem=ag_send.at[0], recv_sem=ag_recv.at[round_of(offset)],
                device_id=dest(peer(offset)), device_id_type=MESH).start()

    gather_start(0)

    def gram_send(stage):
        if stage == 3:
            pltpu.make_async_remote_copy(
                src_ref=gcore.at[core], dst_ref=gcore.at[core],
                send_sem=g_sem.at[4], recv_sem=g_sem.at[3],
                device_id=partner, device_id_type=MESH).start()
            return
        own = mine[stage]
        for off in range(1, sizes[stage]):
            offset = tuple(off if a == stage else 0 for a in range(3))
            pltpu.make_async_remote_copy(
                src_ref=gax.at[stage, own], dst_ref=gax.at[stage, own],
                send_sem=g_sem.at[5 + stage], recv_sem=g_sem.at[stage],
                device_id=dest(peer(offset)), device_id_type=MESH).start()

    def gram_sum(stage):
        if stage == 3:
            for i in (4, 3):
                whole(gcore.at[0], g_sem.at[i]).wait()
            return gcore[0] + gcore[1]
        for i in (5 + stage, stage):
            whole(gax.at[stage, pl.ds(0, sizes[stage] - 1)], g_sem.at[i]).wait()
        total = gax[stage, 0]
        for place in range(1, sizes[stage]):
            total = total + gax[stage, place]
        return total

    gram_send(3)
    whole(x_out, x_sem.at[1]).wait()
    for offset in reversed(offsets):
        c = index(offset, behind)
        pltpu.make_async_remote_copy(
            src_ref=x_out.at[c], dst_ref=x_v.at[c, 2:4],
            send_sem=xr_send.at[0], recv_sem=xr_recv.at[round_of(offset)],
            device_id=partner, device_id_type=MESH).start()
    lab_copy = pltpu.make_async_remote_copy(
        src_ref=lab_send, dst_ref=lab_recv, send_sem=l_sem.at[0], recv_sem=l_sem.at[1],
        device_id=partner, device_id_type=MESH)
    lab_copy.start()

    gax[0, ex] = gram_sum(3)
    gram_send(0)

    row16 = lax.broadcasted_iota(jnp.int32, (16, 128), 0)
    tile16 = lax.broadcasted_iota(jnp.int32, (16, 128), 1) // 8
    on_diag = row16 == tile16
    row24 = lax.broadcasted_iota(jnp.int32, (24, 128), 0)
    lane24 = lax.broadcasted_iota(jnp.int32, (24, 128), 1)
    row_m, lane_m = row24[0:m], lane24[0:m]
    lane1 = lax.broadcasted_iota(jnp.int32, (1, 128), 1)
    eye = jnp.where((row24 == lane24) & (row24 < m), 1.0, 0.0).astype(F32)
    turn = jnp.where(lax.rem(lanes8, 8) == row8, 1.0, 0.0).astype(F32)

    def margin_terms(it, blocks, accs):
        accs = list(accs)
        count = 3 if it == 0 else 4
        if it == 0:
            left = jnp.concatenate([wg[it, c] for c in blocks], axis=1)
            right = jnp.concatenate([x_v[c, 3] for c in blocks], axis=1)
            accs[6] = accs[6] + lax.dot_general(
                left, right, (((1,), (1,)), ((), ())), preferred_element_type=F32)
        for c in blocks:
            for t in range(0, 16, 2):
                w = wg[it, c, t:t + 2, :].astype(F32)
                w = jnp.concatenate(
                    [jnp.broadcast_to(w[0:1], (8, 128)), jnp.broadcast_to(w[1:2], (8, 128))], axis=0)
                for f in range(count):
                    if it == 0:
                        prod = x_v[c, f, t * 8:t * 8 + 16, :].astype(F32) * w
                    else:
                        prod = x_f[c, f, t * 8:t * 8 + 16, :] * w
                    accs[f] = accs[f] + prod[0:8]
                    accs[count + f] = accs[count + f] + prod[8:16]
        return tuple(accs)

    def zeros(count):
        return tuple(jnp.zeros((8, 128), F32) for _ in range(count))

    def lane_sums(accs):
        return [jnp.sum(acc, axis=1, keepdims=True) for acc in accs]

    weights = w_ref[...]
    rinv = rinvt = yy = diag = gamma0 = None
    for it in range(ITERS):
        if it == 0:
            whole(x_out, x_sem.at[0]).wait()

        groups, per = rounds, 1

        def arrive(i, accs):
            g = groups - 1 - i
            if it == 0:
                whole(x_out.at[pl.ds(0, 8 * per)], xr_recv.at[g]).wait()
            whole(wg.at[it, pl.ds(0, 8 * per)], ag_recv.at[g]).wait()
            return lax.fori_loop(
                0, per, lambda j, a: margin_terms(it, round_blocks(g * per + j, behind), a), accs)

        if it == 0:
            accs = arrive(0, zeros(6) + (jnp.zeros((16, 128), F32),))
            gax[1, px] = gram_sum(0)
            gram_send(1)
            accs = lax.fori_loop(1, groups, arrive, accs)
            line = jnp.sum(jnp.where(on_diag, accs[6], 0.0), axis=0, keepdims=True)
            cols = lane_sums([accs[f] + accs[3 + f] for f in range(3)] + [turn * line])
        else:
            accs = lax.fori_loop(0, groups, arrive, zeros(8))
            cols = lane_sums([accs[f] + accs[4 + f] for f in range(4)])
        for k in range(4):
            m_send[it, (k + 2) % 4] = jnp.broadcast_to(cols[k], (8, 128))
        m_copy = pltpu.make_async_remote_copy(
            src_ref=m_send.at[it], dst_ref=m_recv.at[it],
            send_sem=m_sem.at[0], recv_sem=m_sem.at[1],
            device_id=partner, device_id_type=MESH)
        m_copy.start()
        if it > 0:
            whole(ar.at[it - 1, pl.ds(0, 2 * chips - 1)], ar_sem.at[0]).wait()
        if it == 0:
            lab_copy.wait()
            lab_all = [lab_send[0], lab_send[1], lab_recv[0], lab_recv[1]]
        m_copy.wait()
        for k in range(4):
            resid = jax.nn.sigmoid(m_send[it, (k + 2) % 4] + m_recv[it, k]) - lab_all[k]
            line = jnp.sum(turn * resid, axis=0, keepdims=True)
            r_ref[:, k * 128:(k + 1) * 128] = jnp.where(on_diag, line, 0.0).astype(BF16)

        def scatter_send(batch):
            for offset in batch:
                pltpu.make_async_remote_copy(
                    src_ref=rs_send.at[it, index(offset, ahead)], dst_ref=rs_recv.at[it, chip],
                    send_sem=rs_sem.at[0], recv_sem=rs_sem.at[1],
                    device_id=dest(peer(offset)), device_id_type=MESH).start()

        lines = r_ref[...]
        start = 0
        for size in BATCHES[:1] if chips < 16 else BATCHES:
            batch = offsets[start:min(start + size, chips)]
            start += size
            for j in range(0, len(batch), 2):
                c0, c1 = index(batch[j], ahead), index(batch[j + 1], ahead)
                both = jnp.concatenate([x_v[c0].reshape(512, 128), x_v[c1].reshape(512, 128)], axis=1)
                term = jnp.dot(lines, both, preferred_element_type=F32)
                for c, part in ((c0, term[:, 0:128]), (c1, term[:, 128:256])):
                    if it > 0:
                        part = part - rs_send[it - 1, c].astype(F32)
                    rs_send[it, c] = part.astype(BF16)
            scatter_send(batch)
            if it == 0 and start == (BATCHES[0] if chips < 16 else sum(BATCHES[:2])):
                gax[2, pz] = gram_sum(1)
                gram_send(2)
        if it == 0:
            total = gram_sum(2)
            upper = jnp.where((row24 <= lane24) & (lane24 < m), total, 0.0)
            yy = jnp.where((lane24 < m) & (row24 < m), pltpu.roll(total, 64, 1), 0.0)
            diag = upper * eye
            inv = eye
            for i in reversed(range(m)):
                line = inv[i:i + 1, :] / upper[i:i + 1, i:i + 1]
                column = jnp.where(row24[:, 0:1] < i, upper[:, i:i + 1], 0.0)
                inv = jnp.where(row24 == i, line, inv - column * line)
            rinv = inv
            t_ref[0:24, :] = inv
            rinvt = t_ref[...].T[0:24, :]
            gamma0 = upper[m - 1:m, m - 1:m] / yy[m - 1:m, m - 1:m]
        whole(wg.at[it], ag_send.at[0]).wait()
        whole(rs_recv.at[it], rs_sem.at[1]).wait()

        def add(k, total):
            return total + rs_recv[it, k].astype(F32)
        total = lax.fori_loop(0, chips, add, jnp.zeros((16, 128), F32) if it == 0 else data_ref[...], unroll=8)
        if it == 0:
            data_ref[...] = total
        grad = total + 0.1 * weights
        g_ref[...] = grad
        vectors = [g_ref]
        if it > 0:
            gp_ref[...] = grad - gp_ref[...]
            vectors.append(gp_ref)
            for t in range(16):
                y_v[0:1, t * 128:(t + 1) * 128] = gp_ref[t:t + 1, :]
        sums = jnp.zeros((m, 128), F32)
        for v, vec in enumerate(vectors):
            acc_s = jnp.zeros((m, 128), F32)
            acc_y = jnp.zeros((m, 128), F32)
            for t in range(16):
                line = vec[t:t + 1, :]
                acc_s = acc_s + s_v[:, t * 128:(t + 1) * 128] * line
                acc_y = acc_y + y_v[:, t * 128:(t + 1) * 128] * line
            for part, acc in ((2 * v, acc_s), (2 * v + 1, acc_y)):
                own_lane = lane_m == row_m + 32 * part
                sums = sums + jnp.where(own_lane, jnp.sum(acc, axis=1, keepdims=True), 0.0)
        sums = jnp.sum(sums, axis=0, keepdims=True)
        ar_own[it] = sums
        ar[it, chip * 2 + core] = sums

        def total_send(device):
            pltpu.make_async_remote_copy(
                src_ref=ar_own.at[it], dst_ref=ar.at[it, chip * 2 + core],
                send_sem=ar_sem.at[0], recv_sem=ar_sem.at[1],
                device_id=device, device_id_type=MESH).start()

        for offset in offsets[:-1]:
            cy, cxz = peer(offset)
            total_send((cy, cxz * 2))
            total_send((cy, cxz * 2 + 1))
        total_send(partner)
        if it == 0:
            def widen(c, carry):
                x_f[c] = x_v[c].astype(F32)
                return carry
            lax.fori_loop(0, chips, widen, 0)
        whole(rs_send.at[it], rs_sem.at[0]).wait()
        whole(ar.at[it, pl.ds(0, 2 * chips - 1)], ar_sem.at[1]).wait()
        tot = jnp.broadcast_to(jnp.sum(ar[it], axis=0), (8, 128))
        u, hh = tot[0:1], pltpu.roll(tot, 96, 1)[0:1]
        if it == 0:
            gamma = gamma0
            alpha = -jnp.sum(rinv * u, axis=1, keepdims=True)
            p = gamma * (jnp.sum(yy * alpha, axis=0, keepdims=True) + hh)
            p = p + jnp.sum(diag * alpha, axis=0, keepdims=True)
            coef = jnp.sum(rinvt * p, axis=1, keepdims=True)
        else:
            v, z = pltpu.roll(tot, 64, 1)[0:1], pltpu.roll(tot, 32, 1)[0:1]
            v0, z0, u0 = v[:, 0:1], z[:, 0:1], u[:, 0:1]
            gamma = v0 / z0
            a0 = -u0 / v0
            old = (row24 > 0) & (lane24 > 0)
            rm, rmt = jnp.where(old, rinv, 0.0), jnp.where(old, rinvt, 0.0)
            ru = jnp.sum(rm * u, axis=1, keepdims=True)
            rv = jnp.sum(rm * v, axis=1, keepdims=True)
            rv_flat = jnp.sum(eye * rv, axis=0, keepdims=True)
            alpha = jnp.where(row24[:, 0:1] == 0, a0, -(ru + rv * a0))
            flat = jnp.sum(eye * alpha, axis=0, keepdims=True)
            newest = jnp.sum(jnp.where(lane1 < m, z, 0.0) * flat, axis=1, keepdims=True)
            q = jnp.sum(jnp.where(old, yy, 0.0) * alpha, axis=0, keepdims=True) + z * a0
            p = gamma * (q + hh) + jnp.sum(diag * alpha, axis=0, keepdims=True)
            coef = jnp.sum(rmt * p, axis=1, keepdims=True)
            rest = jnp.sum(rv_flat * p, axis=1, keepdims=True)
            c0 = (gamma * (newest + hh[:, 0:1]) + v0 * a0 - rest) / v0
            coef = jnp.where(row24[:, 0:1] == 0, c0, coef)
        cs, cy = coef[0:m], (-gamma * alpha)[0:m]
        for t in range(16):
            cols = slice(t * 128, (t + 1) * 128)
            d_ref[t:t + 1, :] = jnp.sum(cs * s_v[:, cols] + cy * y_v[:, cols], axis=0, keepdims=True)
        direction = d_ref[...] - gamma * g_ref[...]
        new = weights + direction
        if it < ITERS - 1:
            w_own[it + 1] = new.astype(BF16)
            gather_start(it + 1)
            gp_ref[...] = grad
            d_ref[...] = new - weights
            for t in range(16):
                s_v[0:1, t * 128:(t + 1) * 128] = d_ref[t:t + 1, :]
            weights = new
        else:
            out_ref[0] = new
            out_ref[1] = direction

    whole(x_out, xr_send.at[0]).wait()
    whole(ar.at[0, pl.ds(0, 2 * chips - 1)], ar_sem.at[0]).wait()


def per_device(sizes, features, labels, start_weights, hist_s, hist_y):
    ny, nx, nz = sizes
    chips = ny * nx * nz
    m = hist_s.shape[0]
    x = features.reshape(2, 8, chips, 2, 16, 128).transpose(0, 2, 3, 4, 1, 5)
    x = x.reshape(2, chips, 2, 128, 128)
    vmem = pl.BlockSpec(memory_space=pltpu.VMEM)
    hbm = pl.BlockSpec(memory_space=pl.ANY)
    dma = pltpu.SemaphoreType.DMA
    out = pl.pallas_call(
        functools.partial(kernel, sizes),
        out_shape=pltpu.VMEM((2, 16, 128), F32),
        in_specs=[hbm] * 5,
        out_specs=vmem,
        scratch_shapes=[
            pltpu.VMEM((chips, 4, 128, 128), BF16),
            pltpu.VMEM((chips, 2, 128, 128), BF16),
            pltpu.VMEM((chips, 4, 128, 128), F32),
            pltpu.SMEM((16,), jnp.int32),
            pltpu.VMEM((16, 128), F32),
            pltpu.VMEM((m, 2048), F32),
            pltpu.VMEM((m, 2048), F32),
            pltpu.VMEM((ITERS, 16, 128), BF16),
            pltpu.VMEM((ITERS, chips, 16, 128), BF16),
            pltpu.VMEM((ITERS, chips, 16, 128), BF16),
            pltpu.VMEM((ITERS, chips, 16, 128), BF16),
            pltpu.VMEM((ITERS, 1, 128), F32),
            pltpu.VMEM((ITERS, 2 * chips, 1, 128), F32),
            pltpu.VMEM((24, 128), F32),
            pltpu.VMEM((24, 128), F32),
            pltpu.VMEM((2, 24, 128), F32),
            pltpu.VMEM((3, 4, 24, 128), F32),
            pltpu.VMEM((2, 8, 128), F32),
            pltpu.VMEM((2, 8, 128), F32),
            pltpu.VMEM((ITERS, 4, 8, 128), F32),
            pltpu.VMEM((ITERS, 4, 8, 128), F32),
            pltpu.VMEM((16, 512), BF16),
            pltpu.VMEM((128, 128), F32),
            pltpu.VMEM((16, 128), F32),
            pltpu.VMEM((16, 128), F32),
            pltpu.VMEM((16, 128), F32),
            pltpu.VMEM((16, 128), F32),
            dma((2,)), dma((1,)), dma((chips // 8,)), dma((4,)), dma((1,)), dma((chips // 8,)),
            dma((2,)), dma((2,)), dma((8,)), dma((2,)), dma((2,)),
        ],
        compiler_params=pltpu.CompilerParams(collective_id=0, has_side_effects=True),
    )(x, labels, start_weights.reshape(16, 128), hist_s, hist_y)
    out = out.reshape(2, 2048)
    return out[0], out[1]


def solution(mesh):
    ny, rest = mesh.shape["ex"], mesh.shape["ft"] // 2
    nx = round(rest ** 0.5)
    sizes = (ny, nx, rest // nx)
    return jax.shard_map(
        functools.partial(per_device, sizes),
        mesh=mesh,
        in_specs=(
            P(("ex", "ft"), None),
            P(("ex", "ft")),
            P(("ex", "ft")),
            P(None, ("ex", "ft")),
            P(None, ("ex", "ft")),
        ),
        out_specs=(P(("ex", "ft")), P(("ex", "ft"))),
        check_vma=False,
    )
```

```python
import functools
import itertools

import jax
import jax.numpy as jnp
from jax import lax
from jax.experimental import pallas as pl
from jax.experimental.pallas import tpu as pltpu
from jax.sharding import PartitionSpec as P

ITERS = 2
MESH = pl.DeviceIdType.MESH
HI = lax.Precision.HIGHEST
F32 = jnp.float32
BF16 = jnp.bfloat16
BATCHES = (4, 4, 8, 8, 8, 8, 8, 8, 8)


def contract_last(a, b):
    return lax.dot_general(a, b, (((1,), (1,)), ((), ())), precision=HI, preferred_element_type=F32)


def hops(offset, sizes):
    return sum(min(o, n - o) for o, n in zip(offset, sizes))


def kernel(
    sizes, x_hbm, lab_hbm, w_hbm, s_hbm, y_hbm, out_ref,
    x_v, x_out, x_f, lab_ref, w_ref, s_v, y_v, w_own, wg, rs_send, rs_recv, ar_own, ar, gl, gtmp, gcore, gax,
    lab_send, lab_recv, m_send, m_recv, r_ref, t_ref, g_ref, gp_ref, d_ref,
    x_sem, xr_send, xr_recv, h_sem, ag_send, ag_recv, rs_sem, ar_sem, g_sem, l_sem, m_sem,
):
    ny, nx, nz = sizes
    plane = nx * nz
    chips = ny * plane
    m = s_v.shape[0]
    ex = lax.axis_index("ex")
    ft = lax.axis_index("ft")
    core = lax.rem(ft, 2)
    xz = ft // 2
    px, pz = xz // nz, lax.rem(xz, nz)
    chip = ex * plane + xz
    other = 1 - core
    partner = (ex, xz * 2 + other)

    steps = (plane, nz, 1)
    mine = (ex, px, pz)
    ahead = [[lax.rem(p + o, n) * d for o in range(n)] for p, n, d in zip(mine, sizes, steps)]
    behind = [[lax.rem(p + n - o, n) * d for o in range(n)] for p, n, d in zip(mine, sizes, steps)]

    def index(offset, table):
        return table[0][offset[0]] + table[1][offset[1]] + table[2][offset[2]]

    at_y = [lax.rem(ex + o, ny) for o in range(ny)]

    def peer(offset):
        return at_y[offset[0]], ahead[1][offset[1]] + ahead[2][offset[2]]

    def dest(place):
        return (place[0], place[1] * 2 + other)

    offsets = sorted(
        itertools.product(*map(range, sizes)),
        key=lambda o: -hops(o, sizes))
    rounds = chips // 8

    def round_of(offset):
        j = 0
        for o, n in zip(offset, sizes):
            j = 2 * j + (1 if n == 4 and o in (3, 0) else 0)
        return {3: 4, 4: 3}.get(j, j)

    def round_blocks(k, table):
        j = k + jnp.where(k == 3, 1, 0) - jnp.where(k == 4, 1, 0)
        lows = []
        for places, high in zip(table, (j // 4, lax.rem(j // 2, 2), lax.rem(j, 2))):
            if len(places) == 4:
                lows.append([jnp.where(high == 0, places[2], places[3]), jnp.where(high == 0, places[1], places[0])])
            else:
                lows.append([places[1], places[0]])
        return [a + b + c for a in lows[0] for b in lows[1] for c in lows[2]]

    def whole(ref, sem):
        return pltpu.make_async_copy(ref, ref, sem)

    hist = [
        pltpu.make_async_copy(s_hbm, s_v, h_sem.at[0]),
        pltpu.make_async_copy(y_hbm, y_v, h_sem.at[1]),
    ]
    small = [
        pltpu.make_async_copy(w_hbm, w_ref, h_sem.at[2]),
        pltpu.make_async_copy(lab_hbm, lab_ref, h_sem.at[3]),
    ]
    for copy in small + hist:
        copy.start()
    for h in range(2):
        pltpu.make_async_copy(x_hbm.at[h, :, core], x_out.at[:, h], x_sem.at[1]).start()
    for h in range(2):
        pltpu.make_async_copy(x_hbm.at[h, :, other], x_v.at[:, h], x_sem.at[0]).start()

    barrier = pltpu.get_barrier_semaphore()
    for offset in offsets:
        pl.semaphore_signal(barrier, inc=1, device_id=dest(peer(offset)), device_id_type=MESH)

    row8 = lax.broadcasted_iota(jnp.int32, (8, 128), 0)
    lanes8 = lax.broadcasted_iota(jnp.int32, (8, 128), 1)
    for copy in small:
        copy.wait()
    lab = jnp.zeros((8, 128), F32)
    for h in range(2):
        for e in range(8):
            value = lab_ref[h * 8 + e].astype(F32)
            lab = jnp.where((row8 == e), value, lab)
        lab_send[h] = lab
    w_own[0] = w_ref[...].astype(BF16)
    t_ref[...] = jnp.zeros_like(t_ref)
    gl[...] = jnp.zeros_like(gl)
    gtmp[...] = jnp.zeros_like(gtmp)
    for copy in hist:
        copy.wait()
    gl[0:m, 0:m] = contract_last(s_v[...], y_v[...])
    gtmp[0:m, 0:m] = contract_last(y_v[...], y_v[...])
    gcore[core] = gl[...] + pltpu.roll(gtmp[...], 64, 1)
    pl.semaphore_wait(barrier, chips)

    def gather_start(it):
        for offset in offsets:
            pltpu.make_async_remote_copy(
                src_ref=w_own.at[it], dst_ref=wg.at[it, chip],
                send_sem=ag_send.at[0], recv_sem=ag_recv.at[round_of(offset)],
                device_id=dest(peer(offset)), device_id_type=MESH).start()

    gather_start(0)

    def gram_send(stage):
        if stage == 3:
            pltpu.make_async_remote_copy(
                src_ref=gcore.at[core], dst_ref=gcore.at[core],
                send_sem=g_sem.at[4], recv_sem=g_sem.at[3],
                device_id=partner, device_id_type=MESH).start()
            return
        own = mine[stage]
        for off in range(1, sizes[stage]):
            offset = tuple(off if a == stage else 0 for a in range(3))
            pltpu.make_async_remote_copy(
                src_ref=gax.at[stage, own], dst_ref=gax.at[stage, own],
                send_sem=g_sem.at[5 + stage], recv_sem=g_sem.at[stage],
                device_id=dest(peer(offset)), device_id_type=MESH).start()

    def gram_sum(stage):
        if stage == 3:
            for i in (4, 3):
                whole(gcore.at[0], g_sem.at[i]).wait()
            return gcore[0] + gcore[1]
        for i in (5 + stage, stage):
            whole(gax.at[stage, pl.ds(0, sizes[stage] - 1)], g_sem.at[i]).wait()
        total = gax[stage, 0]
        for place in range(1, sizes[stage]):
            total = total + gax[stage, place]
        return total

    gram_send(3)
    whole(x_out, x_sem.at[1]).wait()
    for offset in reversed(offsets):
        c = index(offset, behind)
        pltpu.make_async_remote_copy(
            src_ref=x_out.at[c], dst_ref=x_v.at[c, 2:4],
            send_sem=xr_send.at[0], recv_sem=xr_recv.at[round_of(offset)],
            device_id=partner, device_id_type=MESH).start()
    lab_copy = pltpu.make_async_remote_copy(
        src_ref=lab_send, dst_ref=lab_recv, send_sem=l_sem.at[0], recv_sem=l_sem.at[1],
        device_id=partner, device_id_type=MESH)
    lab_copy.start()

    gax[0, ex] = gram_sum(3)
    gram_send(0)

    row16 = lax.broadcasted_iota(jnp.int32, (16, 128), 0)
    tile16 = lax.broadcasted_iota(jnp.int32, (16, 128), 1) // 8
    on_diag = row16 == tile16
    row24 = lax.broadcasted_iota(jnp.int32, (24, 128), 0)
    lane24 = lax.broadcasted_iota(jnp.int32, (24, 128), 1)
    row_m, lane_m = row24[0:m], lane24[0:m]
    lane1 = lax.broadcasted_iota(jnp.int32, (1, 128), 1)
    eye = jnp.where((row24 == lane24) & (row24 < m), 1.0, 0.0).astype(F32)
    turn = jnp.where(lax.rem(lanes8, 8) == row8, 1.0, 0.0).astype(F32)

    def margin_terms(it, blocks, accs):
        accs = list(accs)
        count = 3 if it == 0 else 4
        if it == 0:
            left = jnp.concatenate([wg[it, c] for c in blocks], axis=1)
            right = jnp.concatenate([x_v[c, 3] for c in blocks], axis=1)
            accs[6] = accs[6] + lax.dot_general(
                left, right, (((1,), (1,)), ((), ())), preferred_element_type=F32)
        for c in blocks:
            for t in range(0, 16, 2):
                w = wg[it, c, t:t + 2, :].astype(F32)
                w = jnp.concatenate(
                    [jnp.broadcast_to(w[0:1], (8, 128)), jnp.broadcast_to(w[1:2], (8, 128))], axis=0)
                for f in range(count):
                    if it == 0:
                        prod = x_v[c, f, t * 8:t * 8 + 16, :].astype(F32) * w
                    else:
                        prod = x_f[c, f, t * 8:t * 8 + 16, :] * w
                    accs[f] = accs[f] + prod[0:8]
                    accs[count + f] = accs[count + f] + prod[8:16]
        return tuple(accs)

    def zeros(count):
        return tuple(jnp.zeros((8, 128), F32) for _ in range(count))

    def lane_sums(accs):
        return [jnp.sum(acc, axis=1, keepdims=True) for acc in accs]

    weights = w_ref[...]
    rinv = rinvt = yy = diag = gamma0 = None
    for it in range(ITERS):
        if it == 0:
            whole(x_out, x_sem.at[0]).wait()

        groups, per = rounds, 1

        def arrive(i, accs):
            g = groups - 1 - i
            if it == 0:
                whole(x_out.at[pl.ds(0, 8 * per)], xr_recv.at[g]).wait()
            whole(wg.at[it, pl.ds(0, 8 * per)], ag_recv.at[g]).wait()
            return lax.fori_loop(
                0, per, lambda j, a: margin_terms(it, round_blocks(g * per + j, behind), a), accs)

        if it == 0:
            accs = arrive(0, zeros(6) + (jnp.zeros((16, 128), F32),))
            gax[1, px] = gram_sum(0)
            gram_send(1)
            accs = lax.fori_loop(1, groups, arrive, accs)
            line = jnp.sum(jnp.where(on_diag, accs[6], 0.0), axis=0, keepdims=True)
            cols = lane_sums([accs[f] + accs[3 + f] for f in range(3)] + [turn * line])
        else:
            accs = lax.fori_loop(0, groups, arrive, zeros(8))
            cols = lane_sums([accs[f] + accs[4 + f] for f in range(4)])
        for k in range(4):
            m_send[it, (k + 2) % 4] = jnp.broadcast_to(cols[k], (8, 128))
        m_copy = pltpu.make_async_remote_copy(
            src_ref=m_send.at[it], dst_ref=m_recv.at[it],
            send_sem=m_sem.at[0], recv_sem=m_sem.at[1],
            device_id=partner, device_id_type=MESH)
        m_copy.start()
        if it > 0:
            whole(ar.at[it - 1, pl.ds(0, 2 * chips - 1)], ar_sem.at[0]).wait()
        if it == 0:
            lab_copy.wait()
            lab_all = [lab_send[0], lab_send[1], lab_recv[0], lab_recv[1]]
        m_copy.wait()
        for k in range(4):
            resid = jax.nn.sigmoid(m_send[it, (k + 2) % 4] + m_recv[it, k]) - lab_all[k]
            line = jnp.sum(turn * resid, axis=0, keepdims=True)
            r_ref[:, k * 128:(k + 1) * 128] = jnp.where(on_diag, line, 0.0).astype(BF16)

        def scatter_send(batch):
            for offset in batch:
                pltpu.make_async_remote_copy(
                    src_ref=rs_send.at[it, index(offset, ahead)], dst_ref=rs_recv.at[it, chip],
                    send_sem=rs_sem.at[0], recv_sem=rs_sem.at[1],
                    device_id=dest(peer(offset)), device_id_type=MESH).start()

        lines = r_ref[...]
        start = 0
        for size in BATCHES[:2] if chips < 16 else BATCHES:
            batch = offsets[start:min(start + size, chips)]
            start += size
            for j in range(0, len(batch), 2):
                c0, c1 = index(batch[j], ahead), index(batch[j + 1], ahead)
                both = jnp.concatenate([x_v[c0].reshape(512, 128), x_v[c1].reshape(512, 128)], axis=1)
                term = jnp.dot(lines, both, preferred_element_type=F32).astype(BF16)
                rs_send[it, c0] = term[:, 0:128]
                rs_send[it, c1] = term[:, 128:256]
            scatter_send(batch)
            if it == 0 and start == (8 if chips < 16 else sum(BATCHES[:3])):
                gax[2, pz] = gram_sum(1)
                gram_send(2)
        if it == 0:
            total = gram_sum(2)
            upper = jnp.where((row24 <= lane24) & (lane24 < m), total, 0.0)
            yy = jnp.where((lane24 < m) & (row24 < m), pltpu.roll(total, 64, 1), 0.0)
            diag = upper * eye
            inv = eye
            for i in reversed(range(m)):
                line = inv[i:i + 1, :] / upper[i:i + 1, i:i + 1]
                column = jnp.where(row24[:, 0:1] < i, upper[:, i:i + 1], 0.0)
                inv = jnp.where(row24 == i, line, inv - column * line)
            rinv = inv
            t_ref[0:24, :] = inv
            rinvt = t_ref[...].T[0:24, :]
            gamma0 = jnp.broadcast_to(upper[m - 1:m, m - 1:m] / yy[m - 1:m, m - 1:m], (24, 128))
        whole(wg.at[it], ag_send.at[0]).wait()
        whole(rs_recv.at[it], rs_sem.at[1]).wait()

        def add(k, total):
            return total + rs_recv[it, k].astype(F32)
        grad = lax.fori_loop(0, chips, add, jnp.zeros((16, 128), F32), unroll=8) + 0.1 * weights
        g_ref[...] = grad
        vectors = [g_ref]
        if it > 0:
            gp_ref[...] = grad - gp_ref[...]
            vectors.append(gp_ref)
            for t in range(16):
                y_v[0:1, t * 128:(t + 1) * 128] = gp_ref[t:t + 1, :]
        sums = jnp.zeros((m, 128), F32)
        for v, vec in enumerate(vectors):
            acc_s = jnp.zeros((m, 128), F32)
            acc_y = jnp.zeros((m, 128), F32)
            for t in range(16):
                line = vec[t:t + 1, :]
                acc_s = acc_s + s_v[:, t * 128:(t + 1) * 128] * line
                acc_y = acc_y + y_v[:, t * 128:(t + 1) * 128] * line
            for part, acc in ((2 * v, acc_s), (2 * v + 1, acc_y)):
                own_lane = lane_m == row_m + 32 * part
                sums = sums + jnp.where(own_lane, jnp.sum(acc, axis=1, keepdims=True), 0.0)
        sums = jnp.sum(sums, axis=0, keepdims=True)
        ar_own[it] = sums
        ar[it, chip * 2 + core] = sums

        def total_send(device):
            pltpu.make_async_remote_copy(
                src_ref=ar_own.at[it], dst_ref=ar.at[it, chip * 2 + core],
                send_sem=ar_sem.at[0], recv_sem=ar_sem.at[1],
                device_id=device, device_id_type=MESH).start()

        for offset in offsets[:-1]:
            cy, cxz = peer(offset)
            total_send((cy, cxz * 2))
            total_send((cy, cxz * 2 + 1))
        total_send(partner)
        if it == 0:
            def widen(c, carry):
                x_f[c] = x_v[c].astype(F32)
                return carry
            lax.fori_loop(0, chips, widen, 0)
        whole(rs_send.at[it], rs_sem.at[0]).wait()
        whole(ar.at[it, pl.ds(0, 2 * chips - 1)], ar_sem.at[1]).wait()
        tot = jnp.broadcast_to(jnp.sum(ar[it], axis=0), (8, 128))
        u, hh = tot[0:1], pltpu.roll(tot, 96, 1)[0:1]
        if it == 0:
            gamma = gamma0
            alpha = -jnp.sum(rinv * u, axis=1, keepdims=True)
            p = gamma[0:1] * (jnp.sum(yy * alpha, axis=0, keepdims=True) + hh)
            p = p + jnp.sum(diag * alpha, axis=0, keepdims=True)
            coef = jnp.sum(rinvt * p, axis=1, keepdims=True)
        else:
            v, z = pltpu.roll(tot, 64, 1)[0:1], pltpu.roll(tot, 32, 1)[0:1]
            v0, z0, u0 = v[:, 0:1], z[:, 0:1], u[:, 0:1]
            gamma = jnp.broadcast_to(v0 / z0, (24, 128))
            a0 = -u0 / v0
            old = (row24 > 0) & (lane24 > 0)
            rm, rmt = jnp.where(old, rinv, 0.0), jnp.where(old, rinvt, 0.0)
            ru = jnp.sum(rm * u, axis=1, keepdims=True)
            rv = jnp.sum(rm * v, axis=1, keepdims=True)
            rv_flat = jnp.sum(eye * rv, axis=0, keepdims=True)
            alpha = jnp.where(row24[:, 0:1] == 0, a0, -(ru + rv * a0))
            flat = jnp.sum(eye * alpha, axis=0, keepdims=True)
            newest = jnp.sum(jnp.where(lane1 < m, z, 0.0) * flat, axis=1, keepdims=True)
            q = jnp.sum(jnp.where(old, yy, 0.0) * alpha, axis=0, keepdims=True) + z * a0
            p = gamma[0:1] * (q + hh) + jnp.sum(diag * alpha, axis=0, keepdims=True)
            coef = jnp.sum(rmt * p, axis=1, keepdims=True)
            rest = jnp.sum(rv_flat * p, axis=1, keepdims=True)
            c0 = (gamma[0:1, 0:1] * (newest + hh[:, 0:1]) + v0 * a0 - rest) / v0
            coef = jnp.where(row24[:, 0:1] == 0, c0, coef)
        cs, cy = coef[0:m], (-gamma * alpha)[0:m]
        for t in range(16):
            cols = slice(t * 128, (t + 1) * 128)
            d_ref[t:t + 1, :] = jnp.sum(cs * s_v[:, cols] + cy * y_v[:, cols], axis=0, keepdims=True)
        direction = d_ref[...] - gamma[0:16] * g_ref[...]
        new = weights + direction
        if it < ITERS - 1:
            w_own[it + 1] = new.astype(BF16)
            gather_start(it + 1)
            gp_ref[...] = grad
            d_ref[...] = new - weights
            for t in range(16):
                s_v[0:1, t * 128:(t + 1) * 128] = d_ref[t:t + 1, :]
            weights = new
        else:
            out_ref[0] = new
            out_ref[1] = direction

    whole(x_out, xr_send.at[0]).wait()
    whole(ar.at[0, pl.ds(0, 2 * chips - 1)], ar_sem.at[0]).wait()


def per_device(sizes, features, labels, start_weights, hist_s, hist_y):
    ny, nx, nz = sizes
    chips = ny * nx * nz
    m = hist_s.shape[0]
    x = features.reshape(2, 8, chips, 2, 16, 128).transpose(0, 2, 3, 4, 1, 5)
    x = x.reshape(2, chips, 2, 128, 128)
    vmem = pl.BlockSpec(memory_space=pltpu.VMEM)
    hbm = pl.BlockSpec(memory_space=pl.ANY)
    dma = pltpu.SemaphoreType.DMA
    out = pl.pallas_call(
        functools.partial(kernel, sizes),
        out_shape=pltpu.VMEM((2, 16, 128), F32),
        in_specs=[hbm] * 5,
        out_specs=vmem,
        scratch_shapes=[
            pltpu.VMEM((chips, 4, 128, 128), BF16),
            pltpu.VMEM((chips, 2, 128, 128), BF16),
            pltpu.VMEM((chips, 4, 128, 128), F32),
            pltpu.SMEM((16,), jnp.int32),
            pltpu.VMEM((16, 128), F32),
            pltpu.VMEM((m, 2048), F32),
            pltpu.VMEM((m, 2048), F32),
            pltpu.VMEM((ITERS, 16, 128), BF16),
            pltpu.VMEM((ITERS, chips, 16, 128), BF16),
            pltpu.VMEM((ITERS, chips, 16, 128), BF16),
            pltpu.VMEM((ITERS, chips, 16, 128), BF16),
            pltpu.VMEM((ITERS, 1, 128), F32),
            pltpu.VMEM((ITERS, 2 * chips, 1, 128), F32),
            pltpu.VMEM((24, 128), F32),
            pltpu.VMEM((24, 128), F32),
            pltpu.VMEM((2, 24, 128), F32),
            pltpu.VMEM((3, 4, 24, 128), F32),
            pltpu.VMEM((2, 8, 128), F32),
            pltpu.VMEM((2, 8, 128), F32),
            pltpu.VMEM((ITERS, 4, 8, 128), F32),
            pltpu.VMEM((ITERS, 4, 8, 128), F32),
            pltpu.VMEM((16, 512), BF16),
            pltpu.VMEM((128, 128), F32),
            pltpu.VMEM((16, 128), F32),
            pltpu.VMEM((16, 128), F32),
            pltpu.VMEM((16, 128), F32),
            dma((2,)), dma((1,)), dma((chips // 8,)), dma((4,)), dma((1,)), dma((chips // 8,)),
            dma((2,)), dma((2,)), dma((8,)), dma((2,)), dma((2,)),
        ],
        compiler_params=pltpu.CompilerParams(collective_id=0, has_side_effects=True),
    )(x, labels, start_weights.reshape(16, 128), hist_s, hist_y)
    out = out.reshape(2, 2048)
    return out[0], out[1]


def solution(mesh):
    ny, rest = mesh.shape["ex"], mesh.shape["ft"] // 2
    nx = round(rest ** 0.5)
    sizes = (ny, nx, rest // nx)
    return jax.shard_map(
        functools.partial(per_device, sizes),
        mesh=mesh,
        in_specs=(
            P(("ex", "ft"), None),
            P(("ex", "ft")),
            P(("ex", "ft")),
            P(None, ("ex", "ft")),
            P(None, ("ex", "ft")),
        ),
        out_specs=(P(("ex", "ft")), P(("ex", "ft"))),
        check_vma=False,
    )
```

```python
import functools
import itertools

import jax
import jax.numpy as jnp
from jax import lax
from jax.experimental import pallas as pl
from jax.experimental.pallas import tpu as pltpu
from jax.sharding import PartitionSpec as P

ITERS = 2
MESH = pl.DeviceIdType.MESH
HI = lax.Precision.HIGHEST
F32 = jnp.float32
BF16 = jnp.bfloat16
BATCHES = (8, 8, 8, 8, 8, 8, 8, 8)


def contract_last(a, b):
    return lax.dot_general(a, b, (((1,), (1,)), ((), ())), precision=HI, preferred_element_type=F32)


def hops(offset, sizes):
    return sum(min(o, n - o) for o, n in zip(offset, sizes))


def kernel(
    sizes, x_hbm, lab_hbm, w_hbm, s_hbm, y_hbm, out_ref,
    x_v, x_out, x_f, lab_ref, w_ref, s_v, y_v, w_own, wg, rs_send, rs_recv, ar_own, ar, gl, gtmp, gcore, gax,
    lab_send, lab_recv, m_send, m_recv, r_ref, t_ref, g_ref, gp_ref, d_ref,
    x_sem, xr_send, xr_recv, h_sem, ag_send, ag_recv, rs_sem, ar_sem, g_sem, l_sem, m_sem,
):
    ny, nx, nz = sizes
    plane = nx * nz
    chips = ny * plane
    m = s_v.shape[0]
    ex = lax.axis_index("ex")
    ft = lax.axis_index("ft")
    core = lax.rem(ft, 2)
    xz = ft // 2
    px, pz = xz // nz, lax.rem(xz, nz)
    chip = ex * plane + xz
    other = 1 - core
    partner = (ex, xz * 2 + other)

    steps = (plane, nz, 1)
    mine = (ex, px, pz)
    ahead = [[lax.rem(p + o, n) * d for o in range(n)] for p, n, d in zip(mine, sizes, steps)]
    behind = [[lax.rem(p + n - o, n) * d for o in range(n)] for p, n, d in zip(mine, sizes, steps)]

    def index(offset, table):
        return table[0][offset[0]] + table[1][offset[1]] + table[2][offset[2]]

    at_y = [lax.rem(ex + o, ny) for o in range(ny)]

    def peer(offset):
        return at_y[offset[0]], ahead[1][offset[1]] + ahead[2][offset[2]]

    def dest(place):
        return (place[0], place[1] * 2 + other)

    offsets = sorted(
        itertools.product(*map(range, sizes)),
        key=lambda o: -hops(o, sizes))
    rounds = chips // 8

    def round_of(offset):
        j = 0
        for o, n in zip(offset, sizes):
            j = 2 * j + (1 if n == 4 and o in (3, 0) else 0)
        return {3: 4, 4: 3}.get(j, j)

    def round_blocks(k, table):
        j = k + jnp.where(k == 3, 1, 0) - jnp.where(k == 4, 1, 0)
        lows = []
        for places, high in zip(table, (j // 4, lax.rem(j // 2, 2), lax.rem(j, 2))):
            if len(places) == 4:
                lows.append([jnp.where(high == 0, places[2], places[3]), jnp.where(high == 0, places[1], places[0])])
            else:
                lows.append([places[1], places[0]])
        return [a + b + c for a in lows[0] for b in lows[1] for c in lows[2]]

    def whole(ref, sem):
        return pltpu.make_async_copy(ref, ref, sem)

    hist = [
        pltpu.make_async_copy(s_hbm, s_v, h_sem.at[0]),
        pltpu.make_async_copy(y_hbm, y_v, h_sem.at[1]),
    ]
    small = [
        pltpu.make_async_copy(w_hbm, w_ref, h_sem.at[2]),
        pltpu.make_async_copy(lab_hbm, lab_ref, h_sem.at[3]),
    ]
    for copy in small + hist:
        copy.start()
    for h in range(2):
        pltpu.make_async_copy(x_hbm.at[h, :, core], x_out.at[:, h], x_sem.at[1]).start()
    for h in range(2):
        pltpu.make_async_copy(x_hbm.at[h, :, other], x_v.at[:, h], x_sem.at[0]).start()

    barrier = pltpu.get_barrier_semaphore()
    for offset in offsets:
        pl.semaphore_signal(barrier, inc=1, device_id=dest(peer(offset)), device_id_type=MESH)

    row8 = lax.broadcasted_iota(jnp.int32, (8, 128), 0)
    lanes8 = lax.broadcasted_iota(jnp.int32, (8, 128), 1)
    for copy in small:
        copy.wait()
    lab = jnp.zeros((8, 128), F32)
    for h in range(2):
        for e in range(8):
            value = lab_ref[h * 8 + e].astype(F32)
            lab = jnp.where((row8 == e), value, lab)
        lab_send[h] = lab
    w_own[0] = w_ref[...].astype(BF16)
    t_ref[...] = jnp.zeros_like(t_ref)
    gl[...] = jnp.zeros_like(gl)
    gtmp[...] = jnp.zeros_like(gtmp)
    for copy in hist:
        copy.wait()
    gl[0:m, 0:m] = contract_last(s_v[...], y_v[...])
    gtmp[0:m, 0:m] = contract_last(y_v[...], y_v[...])
    gcore[core] = gl[...] + pltpu.roll(gtmp[...], 64, 1)
    pl.semaphore_wait(barrier, chips)

    def gather_start(it):
        for offset in offsets:
            pltpu.make_async_remote_copy(
                src_ref=w_own.at[it], dst_ref=wg.at[it, chip],
                send_sem=ag_send.at[0], recv_sem=ag_recv.at[round_of(offset)],
                device_id=dest(peer(offset)), device_id_type=MESH).start()

    gather_start(0)

    def gram_send(stage):
        if stage == 3:
            pltpu.make_async_remote_copy(
                src_ref=gcore.at[core], dst_ref=gcore.at[core],
                send_sem=g_sem.at[4], recv_sem=g_sem.at[3],
                device_id=partner, device_id_type=MESH).start()
            return
        own = mine[stage]
        for off in range(1, sizes[stage]):
            offset = tuple(off if a == stage else 0 for a in range(3))
            pltpu.make_async_remote_copy(
                src_ref=gax.at[stage, own], dst_ref=gax.at[stage, own],
                send_sem=g_sem.at[5 + stage], recv_sem=g_sem.at[stage],
                device_id=dest(peer(offset)), device_id_type=MESH).start()

    def gram_sum(stage):
        if stage == 3:
            for i in (4, 3):
                whole(gcore.at[0], g_sem.at[i]).wait()
            return gcore[0] + gcore[1]
        for i in (5 + stage, stage):
            whole(gax.at[stage, pl.ds(0, sizes[stage] - 1)], g_sem.at[i]).wait()
        total = gax[stage, 0]
        for place in range(1, sizes[stage]):
            total = total + gax[stage, place]
        return total

    gram_send(3)
    whole(x_out, x_sem.at[1]).wait()
    for offset in reversed(offsets):
        c = index(offset, behind)
        pltpu.make_async_remote_copy(
            src_ref=x_out.at[c], dst_ref=x_v.at[c, 2:4],
            send_sem=xr_send.at[0], recv_sem=xr_recv.at[round_of(offset)],
            device_id=partner, device_id_type=MESH).start()
    lab_copy = pltpu.make_async_remote_copy(
        src_ref=lab_send, dst_ref=lab_recv, send_sem=l_sem.at[0], recv_sem=l_sem.at[1],
        device_id=partner, device_id_type=MESH)
    lab_copy.start()

    gax[0, ex] = gram_sum(3)
    gram_send(0)

    row16 = lax.broadcasted_iota(jnp.int32, (16, 128), 0)
    tile16 = lax.broadcasted_iota(jnp.int32, (16, 128), 1) // 8
    on_diag = row16 == tile16
    row24 = lax.broadcasted_iota(jnp.int32, (24, 128), 0)
    lane24 = lax.broadcasted_iota(jnp.int32, (24, 128), 1)
    row_m, lane_m = row24[0:m], lane24[0:m]
    lane1 = lax.broadcasted_iota(jnp.int32, (1, 128), 1)
    eye = jnp.where((row24 == lane24) & (row24 < m), 1.0, 0.0).astype(F32)
    turn = jnp.where(lax.rem(lanes8, 8) == row8, 1.0, 0.0).astype(F32)

    def margin_terms(it, blocks, accs):
        accs = list(accs)
        count = 3 if it == 0 else 4
        if it == 0:
            left = jnp.concatenate([wg[it, c] for c in blocks], axis=1)
            right = jnp.concatenate([x_v[c, 3] for c in blocks], axis=1)
            accs[6] = accs[6] + lax.dot_general(
                left, right, (((1,), (1,)), ((), ())), preferred_element_type=F32)
        for c in blocks:
            for t in range(0, 16, 2):
                w = wg[it, c, t:t + 2, :].astype(F32)
                w = jnp.concatenate(
                    [jnp.broadcast_to(w[0:1], (8, 128)), jnp.broadcast_to(w[1:2], (8, 128))], axis=0)
                for f in range(count):
                    if it == 0:
                        prod = x_v[c, f, t * 8:t * 8 + 16, :].astype(F32) * w
                    else:
                        prod = x_f[c, f, t * 8:t * 8 + 16, :] * w
                    accs[f] = accs[f] + prod[0:8]
                    accs[count + f] = accs[count + f] + prod[8:16]
        return tuple(accs)

    def zeros(count):
        return tuple(jnp.zeros((8, 128), F32) for _ in range(count))

    def lane_sums(accs):
        return [jnp.sum(acc, axis=1, keepdims=True) for acc in accs]

    weights = w_ref[...]
    rinv = rinvt = yy = diag = gamma0 = None
    for it in range(ITERS):
        if it == 0:
            whole(x_out, x_sem.at[0]).wait()

        groups, per = rounds, 1

        def arrive(i, accs):
            g = groups - 1 - i
            if it == 0:
                whole(x_out.at[pl.ds(0, 8 * per)], xr_recv.at[g]).wait()
            whole(wg.at[it, pl.ds(0, 8 * per)], ag_recv.at[g]).wait()
            return lax.fori_loop(
                0, per, lambda j, a: margin_terms(it, round_blocks(g * per + j, behind), a), accs)

        if it == 0:
            accs = arrive(0, zeros(6) + (jnp.zeros((16, 128), F32),))
            gax[1, px] = gram_sum(0)
            gram_send(1)
            accs = lax.fori_loop(1, groups, arrive, accs)
            line = jnp.sum(jnp.where(on_diag, accs[6], 0.0), axis=0, keepdims=True)
            cols = lane_sums([accs[f] + accs[3 + f] for f in range(3)] + [turn * line])
        else:
            accs = lax.fori_loop(0, groups, arrive, zeros(8))
            cols = lane_sums([accs[f] + accs[4 + f] for f in range(4)])
        for k in range(4):
            m_send[it, (k + 2) % 4] = jnp.broadcast_to(cols[k], (8, 128))
        m_copy = pltpu.make_async_remote_copy(
            src_ref=m_send.at[it], dst_ref=m_recv.at[it],
            send_sem=m_sem.at[0], recv_sem=m_sem.at[1],
            device_id=partner, device_id_type=MESH)
        m_copy.start()
        if it > 0:
            whole(ar.at[it - 1, pl.ds(0, 2 * chips - 1)], ar_sem.at[0]).wait()
        if it == 0:
            lab_copy.wait()
            lab_all = [lab_send[0], lab_send[1], lab_recv[0], lab_recv[1]]
        m_copy.wait()
        for k in range(4):
            resid = jax.nn.sigmoid(m_send[it, (k + 2) % 4] + m_recv[it, k]) - lab_all[k]
            line = jnp.sum(turn * resid, axis=0, keepdims=True)
            r_ref[:, k * 128:(k + 1) * 128] = jnp.where(on_diag, line, 0.0).astype(BF16)

        def scatter_send(batch):
            for offset in batch:
                pltpu.make_async_remote_copy(
                    src_ref=rs_send.at[it, index(offset, ahead)], dst_ref=rs_recv.at[it, chip],
                    send_sem=rs_sem.at[0], recv_sem=rs_sem.at[1],
                    device_id=dest(peer(offset)), device_id_type=MESH).start()

        lines = r_ref[...]
        start = 0
        for size in BATCHES[:1] if chips < 16 else BATCHES:
            batch = offsets[start:min(start + size, chips)]
            start += size
            for j in range(0, len(batch), 2):
                c0, c1 = index(batch[j], ahead), index(batch[j + 1], ahead)
                both = jnp.concatenate([x_v[c0].reshape(512, 128), x_v[c1].reshape(512, 128)], axis=1)
                term = jnp.dot(lines, both, preferred_element_type=F32).astype(BF16)
                rs_send[it, c0] = term[:, 0:128]
                rs_send[it, c1] = term[:, 128:256]
            scatter_send(batch)
            if it == 0 and start == (BATCHES[0] if chips < 16 else sum(BATCHES[:2])):
                gax[2, pz] = gram_sum(1)
                gram_send(2)
        if it == 0:
            total = gram_sum(2)
            upper = jnp.where((row24 <= lane24) & (lane24 < m), total, 0.0)
            yy = jnp.where((lane24 < m) & (row24 < m), pltpu.roll(total, 64, 1), 0.0)
            diag = upper * eye
            inv = eye
            for i in reversed(range(m)):
                line = inv[i:i + 1, :] / upper[i:i + 1, i:i + 1]
                column = jnp.where(row24[:, 0:1] < i, upper[:, i:i + 1], 0.0)
                inv = jnp.where(row24 == i, line, inv - column * line)
            rinv = inv
            t_ref[0:24, :] = inv
            rinvt = t_ref[...].T[0:24, :]
            gamma0 = jnp.broadcast_to(upper[m - 1:m, m - 1:m] / yy[m - 1:m, m - 1:m], (24, 128))
        whole(wg.at[it], ag_send.at[0]).wait()
        whole(rs_recv.at[it], rs_sem.at[1]).wait()

        def add(k, total):
            return total + rs_recv[it, k].astype(F32)
        grad = lax.fori_loop(0, chips, add, jnp.zeros((16, 128), F32), unroll=8) + 0.1 * weights
        g_ref[...] = grad
        vectors = [g_ref]
        if it > 0:
            gp_ref[...] = grad - gp_ref[...]
            vectors.append(gp_ref)
            for t in range(16):
                y_v[0:1, t * 128:(t + 1) * 128] = gp_ref[t:t + 1, :]
        sums = jnp.zeros((m, 128), F32)
        for v, vec in enumerate(vectors):
            acc_s = jnp.zeros((m, 128), F32)
            acc_y = jnp.zeros((m, 128), F32)
            for t in range(16):
                line = vec[t:t + 1, :]
                acc_s = acc_s + s_v[:, t * 128:(t + 1) * 128] * line
                acc_y = acc_y + y_v[:, t * 128:(t + 1) * 128] * line
            for part, acc in ((2 * v, acc_s), (2 * v + 1, acc_y)):
                own_lane = lane_m == row_m + 32 * part
                sums = sums + jnp.where(own_lane, jnp.sum(acc, axis=1, keepdims=True), 0.0)
        sums = jnp.sum(sums, axis=0, keepdims=True)
        ar_own[it] = sums
        ar[it, chip * 2 + core] = sums

        def total_send(device):
            pltpu.make_async_remote_copy(
                src_ref=ar_own.at[it], dst_ref=ar.at[it, chip * 2 + core],
                send_sem=ar_sem.at[0], recv_sem=ar_sem.at[1],
                device_id=device, device_id_type=MESH).start()

        for offset in offsets[:-1]:
            cy, cxz = peer(offset)
            total_send((cy, cxz * 2))
            total_send((cy, cxz * 2 + 1))
        total_send(partner)
        if it == 0:
            def widen(c, carry):
                x_f[c] = x_v[c].astype(F32)
                return carry
            lax.fori_loop(0, chips, widen, 0)
        whole(rs_send.at[it], rs_sem.at[0]).wait()
        whole(ar.at[it, pl.ds(0, 2 * chips - 1)], ar_sem.at[1]).wait()
        tot = jnp.broadcast_to(jnp.sum(ar[it], axis=0), (8, 128))
        u, hh = tot[0:1], pltpu.roll(tot, 96, 1)[0:1]
        if it == 0:
            gamma = gamma0
            alpha = -jnp.sum(rinv * u, axis=1, keepdims=True)
            p = gamma[0:1] * (jnp.sum(yy * alpha, axis=0, keepdims=True) + hh)
            p = p + jnp.sum(diag * alpha, axis=0, keepdims=True)
            coef = jnp.sum(rinvt * p, axis=1, keepdims=True)
        else:
            v, z = pltpu.roll(tot, 64, 1)[0:1], pltpu.roll(tot, 32, 1)[0:1]
            v0, z0, u0 = v[:, 0:1], z[:, 0:1], u[:, 0:1]
            gamma = jnp.broadcast_to(v0 / z0, (24, 128))
            a0 = -u0 / v0
            old = (row24 > 0) & (lane24 > 0)
            rm, rmt = jnp.where(old, rinv, 0.0), jnp.where(old, rinvt, 0.0)
            ru = jnp.sum(rm * u, axis=1, keepdims=True)
            rv = jnp.sum(rm * v, axis=1, keepdims=True)
            rv_flat = jnp.sum(eye * rv, axis=0, keepdims=True)
            alpha = jnp.where(row24[:, 0:1] == 0, a0, -(ru + rv * a0))
            flat = jnp.sum(eye * alpha, axis=0, keepdims=True)
            newest = jnp.sum(jnp.where(lane1 < m, z, 0.0) * flat, axis=1, keepdims=True)
            q = jnp.sum(jnp.where(old, yy, 0.0) * alpha, axis=0, keepdims=True) + z * a0
            p = gamma[0:1] * (q + hh) + jnp.sum(diag * alpha, axis=0, keepdims=True)
            coef = jnp.sum(rmt * p, axis=1, keepdims=True)
            rest = jnp.sum(rv_flat * p, axis=1, keepdims=True)
            c0 = (gamma[0:1, 0:1] * (newest + hh[:, 0:1]) + v0 * a0 - rest) / v0
            coef = jnp.where(row24[:, 0:1] == 0, c0, coef)
        cs, cy = coef[0:m], (-gamma * alpha)[0:m]
        for t in range(16):
            cols = slice(t * 128, (t + 1) * 128)
            d_ref[t:t + 1, :] = jnp.sum(cs * s_v[:, cols] + cy * y_v[:, cols], axis=0, keepdims=True)
        direction = d_ref[...] - gamma[0:16] * g_ref[...]
        new = weights + direction
        if it < ITERS - 1:
            w_own[it + 1] = new.astype(BF16)
            gather_start(it + 1)
            gp_ref[...] = grad
            d_ref[...] = new - weights
            for t in range(16):
                s_v[0:1, t * 128:(t + 1) * 128] = d_ref[t:t + 1, :]
            weights = new
        else:
            out_ref[0] = new
            out_ref[1] = direction

    whole(x_out, xr_send.at[0]).wait()
    whole(ar.at[0, pl.ds(0, 2 * chips - 1)], ar_sem.at[0]).wait()


def per_device(sizes, features, labels, start_weights, hist_s, hist_y):
    ny, nx, nz = sizes
    chips = ny * nx * nz
    m = hist_s.shape[0]
    x = features.reshape(2, 8, chips, 2, 16, 128).transpose(0, 2, 3, 4, 1, 5)
    x = x.reshape(2, chips, 2, 128, 128)
    vmem = pl.BlockSpec(memory_space=pltpu.VMEM)
    hbm = pl.BlockSpec(memory_space=pl.ANY)
    dma = pltpu.SemaphoreType.DMA
    out = pl.pallas_call(
        functools.partial(kernel, sizes),
        out_shape=pltpu.VMEM((2, 16, 128), F32),
        in_specs=[hbm] * 5,
        out_specs=vmem,
        scratch_shapes=[
            pltpu.VMEM((chips, 4, 128, 128), BF16),
            pltpu.VMEM((chips, 2, 128, 128), BF16),
            pltpu.VMEM((chips, 4, 128, 128), F32),
            pltpu.SMEM((16,), jnp.int32),
            pltpu.VMEM((16, 128), F32),
            pltpu.VMEM((m, 2048), F32),
            pltpu.VMEM((m, 2048), F32),
            pltpu.VMEM((ITERS, 16, 128), BF16),
            pltpu.VMEM((ITERS, chips, 16, 128), BF16),
            pltpu.VMEM((ITERS, chips, 16, 128), BF16),
            pltpu.VMEM((ITERS, chips, 16, 128), BF16),
            pltpu.VMEM((ITERS, 1, 128), F32),
            pltpu.VMEM((ITERS, 2 * chips, 1, 128), F32),
            pltpu.VMEM((24, 128), F32),
            pltpu.VMEM((24, 128), F32),
            pltpu.VMEM((2, 24, 128), F32),
            pltpu.VMEM((3, 4, 24, 128), F32),
            pltpu.VMEM((2, 8, 128), F32),
            pltpu.VMEM((2, 8, 128), F32),
            pltpu.VMEM((ITERS, 4, 8, 128), F32),
            pltpu.VMEM((ITERS, 4, 8, 128), F32),
            pltpu.VMEM((16, 512), BF16),
            pltpu.VMEM((128, 128), F32),
            pltpu.VMEM((16, 128), F32),
            pltpu.VMEM((16, 128), F32),
            pltpu.VMEM((16, 128), F32),
            dma((2,)), dma((1,)), dma((chips // 8,)), dma((4,)), dma((1,)), dma((chips // 8,)),
            dma((2,)), dma((2,)), dma((8,)), dma((2,)), dma((2,)),
        ],
        compiler_params=pltpu.CompilerParams(collective_id=0, has_side_effects=True),
    )(x, labels, start_weights.reshape(16, 128), hist_s, hist_y)
    out = out.reshape(2, 2048)
    return out[0], out[1]


def solution(mesh):
    ny, rest = mesh.shape["ex"], mesh.shape["ft"] // 2
    nx = round(rest ** 0.5)
    sizes = (ny, nx, rest // nx)
    return jax.shard_map(
        functools.partial(per_device, sizes),
        mesh=mesh,
        in_specs=(
            P(("ex", "ft"), None),
            P(("ex", "ft")),
            P(("ex", "ft")),
            P(None, ("ex", "ft")),
            P(None, ("ex", "ft")),
        ),
        out_specs=(P(("ex", "ft")), P(("ex", "ft"))),
        check_vma=False,
    )
```
